32 devices in a mesh: member: 2 (over y), lat: 4 (over x, core), lon: 4 (over z).
Axes of the slice: x: 2, y: 2, z: 4, core: 2. Of those that a mesh axis runs over, the one named last changes fastest.
Arguments:
- field: bfloat16 [256, 512, 256], P(('member', 'lat'), 'lon'), parts along dimension 0, may hold values from -6 to 6
- mode_table: int32 [48], replicated, may hold values from 0 to 47, as said below
- analysis: bfloat16 [48, 48, 128], P(('lat', 'lon')), as said below
- synthesis: bfloat16 [48, 48, 128], P(('lat', 'lon')), as said below
- mixing: bfloat16 [1, 2, 256, 256], replicated, may hold values from -0.25 to 0.25
- degree_gain: float32 [1, 48, 256], replicated, may hold values from 0.25 to 1.75
- skip_weight: bfloat16 [1, 256, 256], replicated, may hold values from -0.375 to 0.375
Outputs:
- advanced: bfloat16 [256, 512, 256], P(('member', 'lat'), 'lon'), parts along dimension 0
- spectrum: bfloat16 [96, 48, 2, 256], P(('member', 'lat', 'lon')), parts along dimension 0
The draws below stay inside these ranges and needn't reach their ends.
There are 2 independent parts, one for each index of `member`. The reference program is written for one: setup_inputs(seed, part) draws one part's arguments, and reference() takes and returns one part's arrays. A program takes and returns all parts, laid end to end along the dimension named above; an argument that names none is the same for every part. Nothing has to cross between parts.
Inputs may be any that keep to these rules, and one draw needn't show every extreme that they name: A permutation of 0 to 47; slot s of the spectral layout holds zonal wavenumber mode_table[s]. analysis[s, l, j] = weight[j] P(l, m, colat[j]) rounded to bfloat16, with m = mode_table[s], colat[j] = pi (j + 0.5) / 128, weight[j] = 2 pi^2 sin(colat[j]) / 65536, and P the orthonormal associated Legendre function of degree l and order m at cos(colat) without the Condon-Shortley phase, zero for l < m. synthesis[s, l, j] = c P(l, m, colat[j]) rounded to bfloat16, with m = mode_table[s], c = 1 where m = 0 and c = 2 elsewhere, P and colat as for analysis.
All inputs are finite; a program needn't handle non-finite values.
Results may differ from the reference program's by a relative error of at most 0.0062.
Values may be sent and summed in bfloat16 or wider, within the bound.
A program may use at most 64 MiB of HBM per device.

```python
import math
import jax
import jax.numpy as jnp
from jax import lax

C = 256
BLOCKS = 1
NLAT = 128
NLON = 512
MMAX = 48


def table_orders(key):
    return jax.random.permutation(jax.random.fold_in(key, 11), MMAX).astype(jnp.int32)


def colatitudes(length):
    return (jnp.arange(length, dtype=jnp.float32) + 0.5) * (math.pi / length)


def legendre_values(orders):
    colatitude = colatitudes(NLAT)
    morder = orders.astype(jnp.float32)[:, None]
    cosine = jnp.cos(colatitude)[None, :]
    gamma_half = 0.5 * math.log(math.pi) - math.log(2.0)
    norm_part = 0.5 * (jax.scipy.special.gammaln(morder + 1.5) - jax.scipy.special.gammaln(morder + 1.0) - gamma_half)
    first_log = -0.5 * math.log(4.0 * math.pi) + norm_part + morder * jnp.log(jnp.sin(colatitude))[None, :]
    zero_state = jnp.zeros((orders.shape[0], NLAT), jnp.float32)

    def recur_step(carried, degree):
        upper_value, lower_value, log_scale = carried
        beyond = degree > morder
        starting = degree == morder
        square = degree * degree - morder * morder
        coef_first = jnp.sqrt(jnp.maximum(4.0 * degree * degree - 1.0, 1.0) / jnp.maximum(square, 1.0))
        previous = (degree - 1.0) * (degree - 1.0)
        coef_second = jnp.sqrt(jnp.maximum(previous - morder * morder, 0.0) / jnp.maximum(4.0 * previous - 1.0, 1.0))
        new_upper = jnp.where(beyond, coef_first * (cosine * upper_value - coef_second * lower_value), jnp.where(starting, 1.0, 0.0))
        new_lower = jnp.where(beyond, upper_value, 0.0)
        new_log = jnp.where(starting, first_log, log_scale)
        result = new_upper * jnp.exp(new_log)
        largest = jnp.maximum(jnp.abs(new_upper), jnp.abs(new_lower))
        largest = jnp.where(largest > 0, largest, 1.0)
        return ((new_upper / largest, new_lower / largest, new_log + jnp.log(largest)), result)
    _, values = lax.scan(recur_step, (zero_state, zero_state, zero_state), jnp.arange(MMAX, dtype=jnp.float32))
    return (jnp.transpose(values, (1, 0, 2)), colatitude)


def draw_mode_table(key, part):
    return table_orders(key)


def draw_analysis(key, part):
    values, colatitude = legendre_values(table_orders(key))
    weight = 2.0 * math.pi * math.pi / (NLON * NLAT) * jnp.sin(colatitude)
    return (values * weight[None, None, :]).astype(jnp.bfloat16)


def draw_synthesis(key, part):
    orders = table_orders(key)
    values, colatitude = legendre_values(orders)
    factor = jnp.where(orders == 0, 1.0, 2.0).astype(jnp.float32)
    return (values * factor[:, None, None]).astype(jnp.bfloat16)


def shard_levels(stream_key, dims, pieces, least, high):
    def one(position, blocks):
        steps = jax.random.uniform(jax.random.fold_in(jax.random.fold_in(stream_key, 6), position), (blocks,), jnp.float32, least / len(pieces), high / len(pieces))
        return jnp.repeat(jnp.exp(steps), dims[position] // blocks).reshape((-1,) + (1,) * (len(dims) - position - 1))

    loudness = one(*pieces[0])
    for cut in pieces[1:]:
        loudness = loudness * one(*cut)
    return loudness


def bell_draw(key, dims, width, reach, shards=(), kind=jnp.bfloat16):
    values = width * jax.random.normal(key, dims, jnp.float32)
    if shards:
        values = values * shard_levels(key, dims, shards, -0.22, 0.18)
    return jnp.clip(values, -reach, reach).astype(kind)


def setup_inputs(seed: int = 0, part: int = 0) -> dict:
    streams_of = jax.random.split(jax.random.key(seed), 8)
    part_keys = jax.random.split(jax.random.fold_in(streams_of[7], part), 8)
    return {
        "field": bell_draw(part_keys[0], (NLAT, NLON, C), 1.0, 6.0, ((0, 4), (1, 4))),
        "mode_table": draw_mode_table(jax.random.fold_in(streams_of[7], 71), part),
        "analysis": draw_analysis(jax.random.fold_in(streams_of[7], 71), part),
        "synthesis": draw_synthesis(jax.random.fold_in(streams_of[7], 71), part),
        "mixing": bell_draw(streams_of[4], (BLOCKS, 2, C, C), (2 * C) ** -0.5, 0.25),
        "degree_gain": jnp.clip(1.0 + 0.15 * jax.random.normal(streams_of[5], (BLOCKS, MMAX, C), jnp.float32), 0.25, 1.75),
        "skip_weight": bell_draw(streams_of[6], (BLOCKS, C, C), C ** -0.5, 0.375),
    }


def fourier_table(orders, length):
    phases = (orders[:, None] * jnp.arange(length, dtype=jnp.int32)[None, :]) % length
    angles = phases.astype(jnp.float32) * (2.0 * math.pi / length)
    return jnp.stack([jnp.cos(angles), -jnp.sin(angles)], axis=1).reshape(2 * orders.shape[0], length).astype(jnp.bfloat16)


def rounded(values):
    return lax.optimization_barrier(values.astype(jnp.bfloat16)).astype(jnp.float32)


def reference(field, mode_table, analysis, synthesis, mixing, degree_gain, skip_weight):
    highest = lax.Precision.HIGHEST
    orders = mode_table.astype(jnp.int32)
    analysis_wide = analysis.astype(jnp.float32)
    synthesis_wide = synthesis.astype(jnp.float32)
    table = lax.optimization_barrier(fourier_table(orders, NLON)).astype(jnp.float32)
    current = field
    mixed_modes = None
    for layer_index in range(BLOCKS):
        state_wide = current.astype(jnp.float32)
        lat_side = rounded(jnp.einsum("jkc,qk->jqc", state_wide, table, precision=highest))
        lat_data = lat_side.reshape(NLAT, MMAX, 2 * C)
        coefficients = rounded(jnp.einsum("slj,jsx->slx", analysis_wide, lat_data, precision=highest))
        real_part = mixing[layer_index, 0].astype(jnp.float32)
        imag_part = mixing[layer_index, 1].astype(jnp.float32)
        joined = jnp.concatenate([jnp.concatenate([real_part, imag_part], axis=1), jnp.concatenate([-imag_part, real_part], axis=1)], axis=0)
        product = jnp.dot(coefficients.reshape(-1, 2 * C), joined, precision=highest).reshape(MMAX, MMAX, 2, C)
        mixed_modes = (product * degree_gain[layer_index][None, :, None, :]).astype(jnp.bfloat16)
        synthesized = rounded(jnp.einsum("slj,slx->jsx", synthesis_wide, mixed_modes.astype(jnp.float32).reshape(MMAX, MMAX, 2 * C), precision=highest))
        synthesized = synthesized.reshape(NLAT, 2 * MMAX, C)
        spectral = rounded(jnp.einsum("jqc,qk->jkc", synthesized, table, precision=highest))
        direct = jnp.dot(current.reshape(-1, C), skip_weight[layer_index], preferred_element_type=jnp.float32).reshape(NLAT, NLON, C)
        current = (state_wide + jax.nn.gelu(spectral + direct, approximate=False)).astype(jnp.bfloat16)
    return current, mixed_modes
```

```python
import functools
import math

import jax
import jax.numpy as jnp
from jax import lax
from jax.experimental import pallas as pl
from jax.experimental.pallas import tpu as pltpu
from jax.sharding import PartitionSpec as P

ROWS = 16
PITCH = 20
LANES = 128


def fourier_table(orders, first, count, length):
    points = first + jnp.arange(count, dtype=jnp.int32)
    phases = orders[:, None] * points[None, :] % length
    angles = phases.astype(jnp.float32) * (2.0 * math.pi / length)
    return (
        jnp.stack([jnp.cos(angles), -jnp.sin(angles)], axis=1)
        .reshape(2 * orders.shape[0], count)
        .astype(jnp.bfloat16)
    )


def dot(a, b):
    return jnp.dot(a, b, preferred_element_type=jnp.float32)


def dot_t(a, b):
    return lax.dot_general(a, b, (((0,), (0,)), ((), ())), preferred_element_type=jnp.float32)


def spectral_kernel(
    lat_n, lon_n,
    field, table, analysis, synthesis, mixing, gain,
    mixed, returned,
    field_v, wide, outgoing, incoming, made, load_sem, own_sem, send_sem, recv_sem, back_send, back_recv,
):
    lat = lax.axis_index("lat")
    lon = lax.axis_index("lon")
    me = lat * lon_n + lon
    rows, points, channels = field_v.shape
    slots, degrees, _ = analysis.shape
    per = 2 * slots
    offsets = [(a, b) for b in range(lon_n) for a in range(lat_n) if a or b]
    halves = channels // LANES
    blocks = rows // ROWS
    queries = table.shape[0]

    loads = []
    for b in range(blocks):
        part = pl.ds(b * ROWS, ROWS)
        load = pltpu.make_async_copy(field.at[part], field_v.at[part], load_sem.at[b])
        load.start()
        loads.append(load)
    barrier = pltpu.get_barrier_semaphore()

    def peer(a, b):
        return lax.rem(lat + a, lat_n), lax.rem(lon + b, lon_n)

    for a, b in offsets:
        to_lat, to_lon = peer(a, b)
        pl.semaphore_signal(
            barrier, inc=1, device_id={"lat": to_lat, "lon": to_lon}, device_id_type=pl.DeviceIdType.MESH
        )

    transform = table[...]
    for b in range(blocks):
        loads[b].wait()

        @pl.loop(0, ROWS)
        def _(j):
            y = dot(transform, field_v[b * ROWS + j])
            for h in range(halves):
                wide.at[h][pl.ds(j, queries, stride=PITCH), :] = y[:, h * LANES : (h + 1) * LANES]

        @pl.loop(0, queries // 2)
        def _(i):
            base = pl.multiple_of(i * (2 * PITCH), 8)
            for h in range(halves):
                both = wide[h, pl.ds(base, 2 * PITCH), :]
                for u in range(2):
                    outgoing[2 * i + u, b * ROWS : (b + 1) * ROWS, h * LANES : (h + 1) * LANES] = both[
                        u * PITCH : u * PITCH + ROWS
                    ].astype(jnp.bfloat16)

    pl.semaphore_wait(barrier, len(offsets))
    place = lon * lat_n + lat
    sends = []
    for n, (a, b) in enumerate(offsets):
        to_lat, to_lon = peer(a, b)
        copy = pltpu.make_async_remote_copy(
            src_ref=outgoing.at[pl.ds((to_lat * lon_n + to_lon) * per, per)],
            dst_ref=incoming.at[:, place],
            send_sem=send_sem.at[n],
            recv_sem=recv_sem.at[n],
            device_id={"lat": to_lat, "lon": to_lon},
            device_id_type=pl.DeviceIdType.MESH,
        )
        copy.start()
        sends.append(copy)
    own = pltpu.make_async_copy(outgoing.at[pl.ds(me * per, per)], incoming.at[:, place], own_sem)
    own.start()
    own.wait()
    for copy in sends:
        copy.wait_recv()

    real_w = mixing[0]
    imag_w = mixing[1]
    gains = gain[...]
    all_rows = lat_n * rows
    for s in range(slots):
        weights = analysis[s]
        parts = []
        for r in range(2):
            acc = None
            for b in range(lon_n):
                lat_data = incoming[2 * s + r, b * lat_n : (b + 1) * lat_n].reshape(all_rows, channels)
                term = dot(weights, lat_data)
                acc = term if acc is None else acc + term
            parts.append(acc.astype(jnp.bfloat16))
        real = (dot(parts[0], real_w) - dot(parts[1], imag_w)) * gains
        imag = (dot(parts[0], imag_w) + dot(parts[1], real_w)) * gains
        both = [real.astype(jnp.bfloat16), imag.astype(jnp.bfloat16)]
        for r in range(2):
            mixed[s, :, r * channels : (r + 1) * channels] = both[r]
            made[2 * s + r] = (
                dot_t(synthesis[s], both[r]).astype(jnp.bfloat16).reshape(lat_n, rows, channels)
            )

    backs = []
    spot = pl.ds(me * per, per)
    for n, (a, b) in enumerate(offsets):
        to_lat, to_lon = peer(a, b)
        copy = pltpu.make_async_remote_copy(
            src_ref=made.at[:, to_lat],
            dst_ref=returned.at[spot],
            send_sem=back_send.at[n],
            recv_sem=back_recv.at[n],
            device_id={"lat": to_lat, "lon": to_lon},
            device_id_type=pl.DeviceIdType.MESH,
        )
        copy.start()
        backs.append(copy)
    own = pltpu.make_async_copy(made.at[:, lat], returned.at[spot], own_sem)
    own.start()
    own.wait()
    for copy in sends:
        copy.wait_send()
    for copy in backs:
        copy.wait()


def gelu(x):
    return 0.5 * x * (1.0 + lax.erf(x * math.sqrt(0.5)))


def grid_kernel(field, returned, table_t, skip, out, wide):
    rows, points, channels = field.shape
    queries = returned.shape[0]
    halves = channels // LANES

    @pl.loop(0, queries // 2)
    def _(i):
        base = pl.multiple_of(i * (2 * PITCH), 8)
        for u in range(2):
            row = returned[2 * i + u].astype(jnp.float32)
            for h in range(halves):
                wide[h, pl.ds(base + u * PITCH, ROWS), :] = row[:, h * LANES : (h + 1) * LANES]

    transform = table_t[...]
    weights = skip[...]

    @pl.loop(0, ROWS)
    def _(j):
        parts = [wide.at[h][pl.ds(j, queries, stride=PITCH), :] for h in range(halves)]
        values = jnp.concatenate(parts, axis=1).astype(jnp.bfloat16)
        spectral = dot(transform, values).astype(jnp.bfloat16).astype(jnp.float32)
        state = field[j]
        pre = spectral + dot(state, weights)
        out[j] = (state.astype(jnp.float32) + gelu(pre)).astype(jnp.bfloat16)


def per_device(lat_n, lon_n, field, mode_table, analysis, synthesis, mixing, degree_gain, skip_weight):
    rows, points, channels = field.shape
    modes = mode_table.shape[0]
    slots, degrees, all_rows = analysis.shape
    peers = lat_n * lon_n - 1
    queries = 2 * modes
    table = fourier_table(mode_table, lax.axis_index("lon") * points, points, points * lon_n)
    vmem = pl.BlockSpec(memory_space=pltpu.VMEM)
    anywhere = pl.BlockSpec(memory_space=pl.ANY)
    halves = channels // LANES
    mixed, returned = pl.pallas_call(
        functools.partial(spectral_kernel, lat_n, lon_n),
        out_shape=(
            jax.ShapeDtypeStruct((slots, degrees, 2 * channels), jnp.bfloat16),
            jax.ShapeDtypeStruct((queries, rows, channels), jnp.bfloat16),
        ),
        in_specs=[anywhere] + [vmem] * 5,
        out_specs=(vmem, anywhere),
        scratch_shapes=[
            pltpu.VMEM((rows, points, channels), jnp.bfloat16),
            pltpu.VMEM((halves, queries * PITCH, LANES), jnp.float32),
            pltpu.VMEM((queries, rows, channels), jnp.bfloat16),
            pltpu.VMEM((2 * slots, peers + 1, rows, channels), jnp.bfloat16),
            pltpu.VMEM((2 * slots, lat_n, rows, channels), jnp.bfloat16),
            pltpu.SemaphoreType.DMA((rows // ROWS,)),
            pltpu.SemaphoreType.DMA,
            pltpu.SemaphoreType.DMA((peers,)),
            pltpu.SemaphoreType.DMA((peers,)),
            pltpu.SemaphoreType.DMA((peers,)),
            pltpu.SemaphoreType.DMA((peers,)),
        ],
        compiler_params=pltpu.CompilerParams(
            collective_id=0, has_side_effects=True, vmem_limit_bytes=60 * 1024 * 1024
        ),
    )(field, table, analysis, synthesis, mixing[0], degree_gain[0])
    advanced = pl.pallas_call(
        grid_kernel,
        grid=(rows // ROWS,),
        out_shape=jax.ShapeDtypeStruct(field.shape, jnp.bfloat16),
        in_specs=[
            pl.BlockSpec((ROWS, points, channels), lambda i: (i, 0, 0)),
            pl.BlockSpec((queries, ROWS, channels), lambda i: (0, i, 0)),
            pl.BlockSpec((points, queries), lambda i: (0, 0)),
            pl.BlockSpec((channels, channels), lambda i: (0, 0)),
        ],
        out_specs=pl.BlockSpec((ROWS, points, channels), lambda i: (i, 0, 0)),
        scratch_shapes=[pltpu.VMEM((halves, queries * PITCH, LANES), jnp.float32)],
        compiler_params=pltpu.CompilerParams(vmem_limit_bytes=60 * 1024 * 1024),
    )(field, returned, table.T, skip_weight[0])
    return advanced, mixed.reshape(slots, degrees, 2, channels)


def solution(mesh):
    in_specs = (
        P(("member", "lat"), "lon", None),
        P(),
        P(("lat", "lon"), None, None),
        P(("lat", "lon"), None, None),
        P(),
        P(),
        P(),
    )
    out_specs = (P(("member", "lat"), "lon", None), P(("member", "lat", "lon"), None, None, None))
    body = functools.partial(per_device, mesh.shape["lat"], mesh.shape["lon"])
    return jax.shard_map(body, mesh=mesh, in_specs=in_specs, out_specs=out_specs, check_vma=False)
```

```python
import functools
import math

import jax
import jax.numpy as jnp
from jax import lax
from jax.experimental import pallas as pl
from jax.experimental.pallas import tpu as pltpu
from jax.sharding import PartitionSpec as P

ROWS = 16
PITCH = 20
LANES = 128
VMEM_BYTES = 60 * 1024 * 1024


def fourier_table(orders, first, count, length):
    points = first + jnp.arange(count, dtype=jnp.int32)
    phases = orders[:, None] * points[None, :] % length
    angles = phases.astype(jnp.float32) * (2.0 * math.pi / length)
    return (
        jnp.stack([jnp.cos(angles), -jnp.sin(angles)], axis=1)
        .reshape(2 * orders.shape[0], count)
        .astype(jnp.bfloat16)
    )


def dot(a, b):
    return jnp.dot(a, b, preferred_element_type=jnp.float32)


def dot_t(a, b):
    return lax.dot_general(a, b, (((0,), (0,)), ((), ())), preferred_element_type=jnp.float32)


def spectral_kernel(
    lat_n, lon_n,
    field, table, analysis, synthesis, mixing, gain,
    mixed, returned,
    field_v, wide, outgoing, incoming, made, load_sem, own_sem, send_sem, recv_sem, back_send, back_recv,
):
    lat = lax.axis_index("lat")
    lon = lax.axis_index("lon")
    me = lat * lon_n + lon
    rows, points, channels = field_v.shape
    slots, degrees, _ = analysis.shape
    per = 2 * slots
    offsets = [(a, b) for b in range(lon_n) for a in range(lat_n) if a or b]
    halves = channels // LANES
    blocks = rows // ROWS
    queries = table.shape[0]

    loads = []
    for b in range(blocks):
        part = pl.ds(b * ROWS, ROWS)
        load = pltpu.make_async_copy(field.at[part], field_v.at[part], load_sem.at[b])
        load.start()
        loads.append(load)
    barrier = pltpu.get_barrier_semaphore()

    def peer(a, b):
        return lax.rem(lat + a, lat_n), lax.rem(lon + b, lon_n)

    for a, b in offsets:
        to_lat, to_lon = peer(a, b)
        pl.semaphore_signal(
            barrier, inc=1, device_id={"lat": to_lat, "lon": to_lon}, device_id_type=pl.DeviceIdType.MESH
        )

    transform = table[...]
    for b in range(blocks):
        loads[b].wait()

        @pl.loop(0, ROWS)
        def _(j):
            y = dot(transform, field_v[b * ROWS + j])
            for h in range(halves):
                wide.at[h][pl.ds(j, queries, stride=PITCH), :] = y[:, h * LANES : (h + 1) * LANES]

        @pl.loop(0, queries // 2)
        def _(i):
            base = pl.multiple_of(i * (2 * PITCH), 8)
            for h in range(halves):
                both = wide[h, pl.ds(base, 2 * PITCH), :]
                for u in range(2):
                    outgoing[2 * i + u, b * ROWS : (b + 1) * ROWS, h * LANES : (h + 1) * LANES] = both[
                        u * PITCH : u * PITCH + ROWS
                    ].astype(jnp.bfloat16)

    pl.semaphore_wait(barrier, len(offsets))
    place = lon * lat_n + lat
    sends = []
    for n, (a, b) in enumerate(offsets):
        to_lat, to_lon = peer(a, b)
        copy = pltpu.make_async_remote_copy(
            src_ref=outgoing.at[pl.ds((to_lat * lon_n + to_lon) * per, per)],
            dst_ref=incoming.at[:, place],
            send_sem=send_sem.at[n],
            recv_sem=recv_sem.at[n],
            device_id={"lat": to_lat, "lon": to_lon},
            device_id_type=pl.DeviceIdType.MESH,
        )
        copy.start()
        sends.append(copy)
    own = pltpu.make_async_copy(outgoing.at[pl.ds(me * per, per)], incoming.at[:, place], own_sem)
    own.start()
    own.wait()
    for copy in sends:
        copy.wait_recv()

    real_w = mixing[0]
    imag_w = mixing[1]
    gains = gain[...]
    all_rows = lat_n * rows
    for s in range(slots):
        weights = analysis[s]
        parts = []
        for r in range(2):
            acc = None
            for b in range(lon_n):
                lat_data = incoming[2 * s + r, b * lat_n : (b + 1) * lat_n].reshape(all_rows, channels)
                term = dot(weights, lat_data)
                acc = term if acc is None else acc + term
            parts.append(acc.astype(jnp.bfloat16))
        real = (dot(parts[0], real_w) - dot(parts[1], imag_w)) * gains
        imag = (dot(parts[0], imag_w) + dot(parts[1], real_w)) * gains
        both = [real.astype(jnp.bfloat16), imag.astype(jnp.bfloat16)]
        for r in range(2):
            mixed[s, :, r * channels : (r + 1) * channels] = both[r]
            made[2 * s + r] = (
                dot_t(synthesis[s], both[r]).astype(jnp.bfloat16).reshape(lat_n, rows, channels)
            )

    backs = []
    spot = pl.ds(me * per, per)
    for n, (a, b) in enumerate(offsets):
        to_lat, to_lon = peer(a, b)
        copy = pltpu.make_async_remote_copy(
            src_ref=made.at[:, to_lat],
            dst_ref=returned.at[spot],
            send_sem=back_send.at[n],
            recv_sem=back_recv.at[n],
            device_id={"lat": to_lat, "lon": to_lon},
            device_id_type=pl.DeviceIdType.MESH,
        )
        copy.start()
        backs.append(copy)
    own = pltpu.make_async_copy(made.at[:, lat], returned.at[spot], own_sem)
    own.start()
    own.wait()
    for copy in sends:
        copy.wait_send()
    for copy in backs:
        copy.wait()


def staged_kernel(
    lat_n, lon_n,
    field, table, analysis, synthesis, mixing, gain,
    mixed, returned,
    field_v, wide, outgoing, gathered, analysis_all, synthesis_all, part_out, part_in, mixed_all, made,
    load_sem, own_sem, table_send, table_recv, lat_send, lat_recv, lon_send, lon_recv,
    mix_send, mix_recv, back_send, back_recv,
):
    lat = lax.axis_index("lat")
    lon = lax.axis_index("lon")
    rows, points, channels = field_v.shape
    slots, degrees, _ = analysis.shape
    per = 2 * slots
    all_rows = lat_n * rows
    order = list(range(1, lon_n))[::-1] + [0]

    def at_lat(a):
        return lax.rem(lat + a, lat_n)

    def at_lon(b):
        return lax.rem(lon + b + lon_n, lon_n)

    def remote(src, dst, send, recv, to_lat, to_lon):
        copy = pltpu.make_async_remote_copy(
            src_ref=src, dst_ref=dst, send_sem=send, recv_sem=recv,
            device_id={"lat": to_lat, "lon": to_lon}, device_id_type=pl.DeviceIdType.MESH,
        )
        copy.start()
        return copy

    loads = []
    for b in range(rows // ROWS):
        part = pl.ds(b * ROWS, ROWS)
        load = pltpu.make_async_copy(field.at[part], field_v.at[part], load_sem.at[b])
        load.start()
        loads.append(load)
    barrier = pltpu.get_barrier_semaphore()
    peers = [(at_lat(a), lon) for a in range(1, lat_n)] + [(lat, at_lon(b)) for b in range(1, lon_n)]
    for to_lat, to_lon in peers:
        pl.semaphore_signal(
            barrier, inc=1, device_id={"lat": to_lat, "lon": to_lon}, device_id_type=pl.DeviceIdType.MESH
        )

    tables = []
    transform = table[...]
    for b in range(rows // ROWS):
        loads[b].wait()
        forward_rows(transform, field_v, wide, b)
        if b == 0:
            pl.semaphore_wait(barrier, len(peers))
            for k in range(1, lon_n):
                for t, (src, dst) in enumerate(((analysis, analysis_all), (synthesis, synthesis_all))):
                    tables.append(
                        remote(src, dst.at[k], table_send.at[t, k], table_recv.at[t, k], lat, at_lon(-k))
                    )
        relay_rows(wide, outgoing, b, lat_n, lon_n, per)

    lat_copies = {}
    for b in order:
        target = at_lon(b)
        own = pltpu.make_async_copy(outgoing.at[lat, target], gathered.at[b, :, lat], own_sem.at[b])
        copies = [
            remote(
                outgoing.at[at_lat(a), target], gathered.at[b, :, lat],
                lat_send.at[b, a], lat_recv.at[b, a], at_lat(a), lon,
            )
            for a in range(1, lat_n)
        ]
        own.start()
        lat_copies[b] = (own, copies)

    lon_copies = []
    kept = []
    for b in order:
        own, copies = lat_copies[b]
        own.wait()
        for copy in copies:
            copy.wait_recv()
        if b:
            tables[2 * (b - 1)].wait_recv()
        for s in range(slots):
            weights = analysis_all[b, s] if b else analysis[s]
            for r in range(2):
                value = dot(weights, gathered[b, 2 * s + r].reshape(all_rows, channels))
                if b:
                    part_out[b, s, :, r * channels : (r + 1) * channels] = value.astype(jnp.bfloat16)
                else:
                    kept.append(value)
        if b:
            lon_copies.append(
                remote(part_out.at[b], part_in.at[b], lon_send.at[b], lon_recv.at[b], lat, at_lon(b))
            )
    for copy in lon_copies:
        copy.wait_recv()

    real_w = mixing[0]
    imag_w = mixing[1]
    gains = gain[...]
    for s in range(slots):
        parts = []
        for r in range(2):
            total = kept[2 * s + r]
            for b in range(1, lon_n):
                total = total + part_in[b, s, :, r * channels : (r + 1) * channels].astype(jnp.float32)
            parts.append(total.astype(jnp.bfloat16))
        real = (dot(parts[0], real_w) - dot(parts[1], imag_w)) * gains
        imag = (dot(parts[0], imag_w) + dot(parts[1], real_w)) * gains
        mixed[s, :, :channels] = real.astype(jnp.bfloat16)
        mixed[s, :, channels:] = imag.astype(jnp.bfloat16)

    mix_copies = {
        b: remote(mixed, mixed_all.at[b], mix_send.at[b], mix_recv.at[b], lat, at_lon(-b))
        for b in range(1, lon_n)
    }
    backs = []
    owns = []
    for b in range(lon_n):
        if b:
            mix_copies[b].wait_recv()
            tables[2 * (b - 1) + 1].wait_recv()
        for s in range(slots):
            weights = synthesis_all[b, s] if b else synthesis[s]
            values = dot_t(weights, mixed_all[b, s] if b else mixed[s]).astype(jnp.bfloat16)
            for r in range(2):
                for a in range(lat_n):
                    made[a, b, 2 * s + r] = values[a * rows : (a + 1) * rows, r * channels : (r + 1) * channels]
        spot = pl.ds((lat * lon_n + at_lon(b)) * per, per)
        for a in range(1, lat_n):
            backs.append(
                remote(
                    made.at[at_lat(a), b], returned.at[spot],
                    back_send.at[b, a], back_recv.at[b, a], at_lat(a), lon,
                )
            )
        own = pltpu.make_async_copy(made.at[lat, b], returned.at[spot], own_sem.at[b])
        own.start()
        owns.append(own)
    for own in owns:
        own.wait()
    for copy in tables + [c for b in order for c in lat_copies[b][1]] + lon_copies + list(mix_copies.values()):
        copy.wait_send()
    for copy in backs:
        copy.wait()


def forward_rows(transform, field_v, wide, b):
    queries = transform.shape[0]

    @pl.loop(0, ROWS, unroll=2)
    def _(j):
        y = dot(transform, field_v[b * ROWS + j])
        for h in range(wide.shape[0]):
            wide.at[h][pl.ds(j, queries, stride=PITCH), :] = y[:, h * LANES : (h + 1) * LANES]


def relay_rows(wide, outgoing, b, lat_n, lon_n, per):
    @pl.loop(0, lat_n * lon_n)
    def _(d):
        a = d // lon_n
        k = lax.rem(d, lon_n)
        for i in range(per // 2):
            base = pl.multiple_of((d * (per // 2) + i) * (2 * PITCH), 8)
            for h in range(wide.shape[0]):
                both = wide[h, pl.ds(base, 2 * PITCH), :]
                for u in range(2):
                    outgoing[
                        a, k, 2 * i + u, b * ROWS : (b + 1) * ROWS, h * LANES : (h + 1) * LANES
                    ] = both[u * PITCH : u * PITCH + ROWS].astype(jnp.bfloat16)


def gelu(x):
    return 0.5 * x * (1.0 + lax.erf(x * math.sqrt(0.5)))


def grid_kernel(field, returned, table_t, skip, out, wide):
    rows, points, channels = field.shape
    queries = returned.shape[0]
    halves = channels // LANES

    @pl.loop(0, queries // 2)
    def _(i):
        base = pl.multiple_of(i * (2 * PITCH), 8)
        for u in range(2):
            row = returned[2 * i + u].astype(jnp.float32)
            for h in range(halves):
                wide[h, pl.ds(base + u * PITCH, ROWS), :] = row[:, h * LANES : (h + 1) * LANES]

    transform = table_t[...]
    weights = skip[...]

    @pl.loop(0, ROWS, unroll=2)
    def _(j):
        parts = [wide.at[h][pl.ds(j, queries, stride=PITCH), :] for h in range(halves)]
        values = jnp.concatenate(parts, axis=1).astype(jnp.bfloat16)
        spectral = dot(transform, values).astype(jnp.bfloat16).astype(jnp.float32)
        state = field[j]
        pre = spectral + dot(state, weights)
        out[j] = (state.astype(jnp.float32) + gelu(pre)).astype(jnp.bfloat16)


def per_device(lat_n, lon_n, field, mode_table, analysis, synthesis, mixing, degree_gain, skip_weight):
    rows, points, channels = field.shape
    modes = mode_table.shape[0]
    slots, degrees, all_rows = analysis.shape
    peers = lat_n * lon_n - 1
    queries = 2 * modes
    table = fourier_table(mode_table, lax.axis_index("lon") * points, points, points * lon_n)
    vmem = pl.BlockSpec(memory_space=pltpu.VMEM)
    anywhere = pl.BlockSpec(memory_space=pl.ANY)
    halves = channels // LANES
    wide = pltpu.VMEM((halves, queries * PITCH, LANES), jnp.float32)
    exchanged = (lat_n, lon_n, 2 * slots, rows, channels)
    coded = (lon_n, slots, degrees, 2 * channels)
    weights = (lon_n,) + analysis.shape
    staged = [
        ((rows, points, channels), jnp.bfloat16),
        (exchanged, jnp.bfloat16),
        ((lon_n, 2 * slots, lat_n, rows, channels), jnp.bfloat16),
        (weights, jnp.bfloat16),
        (weights, jnp.bfloat16),
        (coded, jnp.bfloat16),
        (coded, jnp.bfloat16),
        (coded, jnp.bfloat16),
        (exchanged, jnp.bfloat16),
    ]
    held = sum(2 * math.prod(shape) for shape, _ in staged) + 4 * halves * queries * PITCH * LANES
    dma = pltpu.SemaphoreType.DMA
    if held < VMEM_BYTES * 3 // 4:
        kernel = staged_kernel
        buffers = [pltpu.VMEM(shape, dtype) for shape, dtype in staged]
        scratch = [buffers[0], wide] + buffers[1:] + [
            dma((rows // ROWS,)),
            dma((lon_n,)),
            dma((2, lon_n)),
            dma((2, lon_n)),
            dma((lon_n, lat_n)),
            dma((lon_n, lat_n)),
            dma((lon_n,)),
            dma((lon_n,)),
            dma((lon_n,)),
            dma((lon_n,)),
            dma((lon_n, lat_n)),
            dma((lon_n, lat_n)),
        ]
    else:
        kernel = spectral_kernel
        scratch = [
            pltpu.VMEM((rows, points, channels), jnp.bfloat16),
            wide,
            pltpu.VMEM((queries, rows, channels), jnp.bfloat16),
            pltpu.VMEM((2 * slots, peers + 1, rows, channels), jnp.bfloat16),
            pltpu.VMEM((2 * slots, lat_n, rows, channels), jnp.bfloat16),
            dma((rows // ROWS,)),
            dma,
        ] + [dma((peers,))] * 4
    mixed, returned = pl.pallas_call(
        functools.partial(kernel, lat_n, lon_n),
        out_shape=(
            jax.ShapeDtypeStruct((slots, degrees, 2 * channels), jnp.bfloat16),
            jax.ShapeDtypeStruct((queries, rows, channels), jnp.bfloat16),
        ),
        in_specs=[anywhere] + [vmem] * 5,
        out_specs=(vmem, anywhere),
        scratch_shapes=scratch,
        compiler_params=pltpu.CompilerParams(
            collective_id=0, has_side_effects=True, vmem_limit_bytes=VMEM_BYTES
        ),
    )(field, table, analysis, synthesis, mixing[0], degree_gain[0])
    advanced = pl.pallas_call(
        grid_kernel,
        grid=(rows // ROWS,),
        out_shape=jax.ShapeDtypeStruct(field.shape, jnp.bfloat16),
        in_specs=[
            pl.BlockSpec((ROWS, points, channels), lambda i: (i, 0, 0)),
            pl.BlockSpec((queries, ROWS, channels), lambda i: (0, i, 0)),
            pl.BlockSpec((points, queries), lambda i: (0, 0)),
            pl.BlockSpec((channels, channels), lambda i: (0, 0)),
        ],
        out_specs=pl.BlockSpec((ROWS, points, channels), lambda i: (i, 0, 0)),
        scratch_shapes=[pltpu.VMEM((halves, queries * PITCH, LANES), jnp.float32)],
        compiler_params=pltpu.CompilerParams(vmem_limit_bytes=VMEM_BYTES),
    )(field, returned, table.T, skip_weight[0])
    return advanced, mixed.reshape(slots, degrees, 2, channels)


def solution(mesh):
    in_specs = (
        P(("member", "lat"), "lon", None),
        P(),
        P(("lat", "lon"), None, None),
        P(("lat", "lon"), None, None),
        P(),
        P(),
        P(),
    )
    out_specs = (P(("member", "lat"), "lon", None), P(("member", "lat", "lon"), None, None, None))
    body = functools.partial(per_device, mesh.shape["lat"], mesh.shape["lon"])
    return jax.shard_map(body, mesh=mesh, in_specs=in_specs, out_specs=out_specs, check_vma=False)
```

```python
import functools
import math

import jax
import jax.numpy as jnp
from jax import lax
from jax.experimental import pallas as pl
from jax.experimental.pallas import tpu as pltpu
from jax.sharding import PartitionSpec as P

ROWS = 16
PITCH = 20
LANES = 128
VMEM_BYTES = 60 * 1024 * 1024


def fourier_table(orders, first, count, length):
    points = first + jnp.arange(count, dtype=jnp.int32)
    phases = orders[:, None] * points[None, :] % length
    angles = phases.astype(jnp.float32) * (2.0 * math.pi / length)
    return (
        jnp.stack([jnp.cos(angles), -jnp.sin(angles)], axis=1)
        .reshape(2 * orders.shape[0], count)
        .astype(jnp.bfloat16)
    )


def dot(a, b):
    return jnp.dot(a, b, preferred_element_type=jnp.float32)


def dot_t(a, b):
    return lax.dot_general(a, b, (((0,), (0,)), ((), ())), preferred_element_type=jnp.float32)


def spectral_kernel(
    lat_n, lon_n,
    field, table, analysis, synthesis, mixing, gain,
    mixed, returned,
    field_v, wide, outgoing, incoming, made, load_sem, own_sem, send_sem, recv_sem, back_send, back_recv,
):
    lat = lax.axis_index("lat")
    lon = lax.axis_index("lon")
    me = lat * lon_n + lon
    rows, points, channels = field_v.shape
    slots, degrees, _ = analysis.shape
    per = 2 * slots
    offsets = [(a, b) for b in range(lon_n) for a in range(lat_n) if a or b]
    halves = channels // LANES
    blocks = rows // ROWS
    queries = table.shape[0]

    loads = []
    for b in range(blocks):
        part = pl.ds(b * ROWS, ROWS)
        load = pltpu.make_async_copy(field.at[part], field_v.at[part], load_sem.at[b])
        load.start()
        loads.append(load)
    barrier = pltpu.get_barrier_semaphore()

    def peer(a, b):
        return lax.rem(lat + a, lat_n), lax.rem(lon + b, lon_n)

    for a, b in offsets:
        to_lat, to_lon = peer(a, b)
        pl.semaphore_signal(
            barrier, inc=1, device_id={"lat": to_lat, "lon": to_lon}, device_id_type=pl.DeviceIdType.MESH
        )

    transform = table[...]
    for b in range(blocks):
        loads[b].wait()

        @pl.loop(0, ROWS)
        def _(j):
            y = dot(transform, field_v[b * ROWS + j])
            for h in range(halves):
                wide.at[h][pl.ds(j, queries, stride=PITCH), :] = y[:, h * LANES : (h + 1) * LANES]

        @pl.loop(0, queries // 2)
        def _(i):
            base = pl.multiple_of(i * (2 * PITCH), 8)
            for h in range(halves):
                both = wide[h, pl.ds(base, 2 * PITCH), :]
                for u in range(2):
                    outgoing[2 * i + u, b * ROWS : (b + 1) * ROWS, h * LANES : (h + 1) * LANES] = both[
                        u * PITCH : u * PITCH + ROWS
                    ].astype(jnp.bfloat16)

    pl.semaphore_wait(barrier, len(offsets))
    place = lon * lat_n + lat
    sends = []
    for n, (a, b) in enumerate(offsets):
        to_lat, to_lon = peer(a, b)
        copy = pltpu.make_async_remote_copy(
            src_ref=outgoing.at[pl.ds((to_lat * lon_n + to_lon) * per, per)],
            dst_ref=incoming.at[:, place],
            send_sem=send_sem.at[n],
            recv_sem=recv_sem.at[n],
            device_id={"lat": to_lat, "lon": to_lon},
            device_id_type=pl.DeviceIdType.MESH,
        )
        copy.start()
        sends.append(copy)
    own = pltpu.make_async_copy(outgoing.at[pl.ds(me * per, per)], incoming.at[:, place], own_sem)
    own.start()
    own.wait()
    for copy in sends:
        copy.wait_recv()

    real_w = mixing[0]
    imag_w = mixing[1]
    gains = gain[...]
    all_rows = lat_n * rows
    for s in range(slots):
        weights = analysis[s]
        parts = []
        for r in range(2):
            acc = None
            for b in range(lon_n):
                lat_data = incoming[2 * s + r, b * lat_n : (b + 1) * lat_n].reshape(all_rows, channels)
                term = dot(weights, lat_data)
                acc = term if acc is None else acc + term
            parts.append(acc.astype(jnp.bfloat16))
        real = (dot(parts[0], real_w) - dot(parts[1], imag_w)) * gains
        imag = (dot(parts[0], imag_w) + dot(parts[1], real_w)) * gains
        both = [real.astype(jnp.bfloat16), imag.astype(jnp.bfloat16)]
        for r in range(2):
            mixed[s, :, r * channels : (r + 1) * channels] = both[r]
            made[2 * s + r] = (
                dot_t(synthesis[s], both[r]).astype(jnp.bfloat16).reshape(lat_n, rows, channels)
            )

    backs = []
    spot = pl.ds(me * per, per)
    for n, (a, b) in enumerate(offsets):
        to_lat, to_lon = peer(a, b)
        copy = pltpu.make_async_remote_copy(
            src_ref=made.at[:, to_lat],
            dst_ref=returned.at[spot],
            send_sem=back_send.at[n],
            recv_sem=back_recv.at[n],
            device_id={"lat": to_lat, "lon": to_lon},
            device_id_type=pl.DeviceIdType.MESH,
        )
        copy.start()
        backs.append(copy)
    own = pltpu.make_async_copy(made.at[:, lat], returned.at[spot], own_sem)
    own.start()
    own.wait()
    for copy in sends:
        copy.wait_send()
    for copy in backs:
        copy.wait()


def staged_kernel(
    lat_n, lon_n,
    field, table, analysis, synthesis, mixing, gain,
    mixed, returned,
    field_v, wide, outgoing, gathered, analysis_all, synthesis_all, part_out, part_in, mixed_all, made, landing, packed,
    load_sem, own_sem, table_send, table_recv, lat_send, lat_recv, lon_send, lon_recv,
    mix_send, mix_recv, back_send, back_recv, out_sem,
):
    lat = lax.axis_index("lat")
    lon = lax.axis_index("lon")
    rows, points, channels = field_v.shape
    slots, degrees, _ = analysis.shape
    per = 2 * slots
    all_rows = lat_n * rows
    order = sorted(range(1, lon_n), key=lambda k: abs(2 * k - lon_n)) + [0]
    blocks = rows // ROWS
    halves = channels // LANES
    early = order[: lon_n // 2] if blocks > 1 else []

    def at_lat(a):
        return lax.rem(lat + a, lat_n)

    def at_lon(b):
        return lax.rem(lon + b + lon_n, lon_n)

    def remote(src, dst, send, recv, to_lat, to_lon):
        copy = pltpu.make_async_remote_copy(
            src_ref=src, dst_ref=dst, send_sem=send, recv_sem=recv,
            device_id={"lat": to_lat, "lon": to_lon}, device_id_type=pl.DeviceIdType.MESH,
        )
        copy.start()
        return copy

    loads = []
    for b in range(rows // ROWS):
        part = pl.ds(b * ROWS, ROWS)
        load = pltpu.make_async_copy(field.at[part], field_v.at[part], load_sem.at[b])
        load.start()
        loads.append(load)
    barrier = pltpu.get_barrier_semaphore()
    peers = [(at_lat(a), lon) for a in range(1, lat_n)] + [(lat, at_lon(b)) for b in range(1, lon_n)]
    for to_lat, to_lon in peers:
        pl.semaphore_signal(
            barrier, inc=1, device_id={"lat": to_lat, "lon": to_lon}, device_id_type=pl.DeviceIdType.MESH
        )

    def to_owners(b, part, index):
        target = at_lon(b)
        return [
            remote(
                outgoing.at[at_lat(a), target, :, part], gathered.at[b, :, lat, part],
                lat_send.at[index, b, a], lat_recv.at[index, b, a], at_lat(a), lon,
            )
            for a in range(1, lat_n)
        ]

    tables = {}
    lat_copies = {b: [] for b in order}
    transform = table[...]
    for b in range(blocks):
        loads[b].wait()
        slabs = wide.at[pl.ds(b * halves, halves)]
        forward_rows(transform, field_v, slabs, b)
        relay_rows(slabs, outgoing, b, lat_n, lon_n, per)
        if b == 0:
            pl.semaphore_wait(barrier, len(peers))
        for k in early:
            lat_copies[k] += to_owners(k, pl.ds(b * ROWS, ROWS), b)
        if b == 0:
            for t, (src, dst) in enumerate(((analysis, analysis_all), (synthesis, synthesis_all))):
                for k in order[:-1]:
                    tables[t, k] = remote(
                        src, dst.at[k], table_send.at[t, k], table_recv.at[t, k], lat, at_lon(-k)
                    )
    owns = {}
    for b in order:
        if b not in early:
            lat_copies[b] += to_owners(b, pl.ds(0, rows), 0)
        owns[b] = pltpu.make_async_copy(outgoing.at[lat, at_lon(b)], gathered.at[b, :, lat], own_sem.at[b])
        owns[b].start()

    lon_copies = []
    kept = []
    for b in order:
        owns[b].wait()
        for copy in lat_copies[b]:
            copy.wait_recv()
        if b:
            tables[0, b].wait_recv()
        for s in range(slots):
            weights = analysis_all[b, s] if b else analysis[s]
            for r in range(2):
                value = dot(weights, gathered[b, 2 * s + r].reshape(all_rows, channels))
                if b:
                    part_out[b, s, :, r * channels : (r + 1) * channels] = value.astype(jnp.bfloat16)
                else:
                    kept.append(value)
        if b:
            lon_copies.append(
                remote(part_out.at[b], part_in.at[b], lon_send.at[b], lon_recv.at[b], lat, at_lon(b))
            )
    for copy in lon_copies:
        copy.wait_recv()

    real_w = mixing[0]
    imag_w = mixing[1]
    gains = gain[...]
    for s in range(slots):
        parts = []
        for r in range(2):
            total = kept[2 * s + r]
            for b in range(1, lon_n):
                total = total + part_in[b, s, :, r * channels : (r + 1) * channels].astype(jnp.float32)
            parts.append(total.astype(jnp.bfloat16))
        real = (dot(parts[0], real_w) - dot(parts[1], imag_w)) * gains
        imag = (dot(parts[0], imag_w) + dot(parts[1], real_w)) * gains
        mixed[s, :, :channels] = real.astype(jnp.bfloat16)
        mixed[s, :, channels:] = imag.astype(jnp.bfloat16)

    back_order = order[::-1]
    mix_copies = {
        b: remote(mixed, mixed_all.at[b], mix_send.at[b], mix_recv.at[b], lat, at_lon(-b))
        for b in back_order[1:]
    }
    backs = {}
    for b in back_order:
        if b:
            mix_copies[b].wait_recv()
            tables[1, b].wait_recv()
        for s in range(slots):
            weights = synthesis_all[b, s] if b else synthesis[s]
            values = dot_t(weights, mixed_all[b, s] if b else mixed[s]).astype(jnp.bfloat16)
            for r in range(2):
                for a in range(lat_n):
                    made[a, b, 2 * s + r] = values[a * rows : (a + 1) * rows, r * channels : (r + 1) * channels]
        for a in range(1, lat_n):
            backs[b, a] = remote(
                made.at[at_lat(a), b], landing.at[b, a],
                back_send.at[b, a], back_recv.at[b, a], at_lat(a), lon,
            )
        owns[b] = pltpu.make_async_copy(made.at[lat, b], landing.at[b, 0], own_sem.at[b])
        owns[b].start()

    for b in back_order:
        owns[b].wait()
        for a in range(1, lat_n):
            backs[b, a].wait_recv()
        for a in range(lat_n):
            source = at_lat(lat_n - a) * lon_n + at_lon(b)
            base = pl.multiple_of(source * (per * PITCH), 8)
            for i in range(per):
                values = landing[b, a, i].astype(jnp.float32)
                for c in range(blocks):
                    for h in range(halves):
                        wide[c * halves + h, pl.ds(base + i * PITCH, ROWS), :] = values[
                            c * ROWS : (c + 1) * ROWS, h * LANES : (h + 1) * LANES
                        ]

    queries = table.shape[0]
    outs = []
    for c in range(blocks):

        @pl.loop(0, ROWS, unroll=4)
        def _(j):
            for h in range(halves):
                packed[c * ROWS + j, :, h * LANES : (h + 1) * LANES] = wide.at[c * halves + h][
                    pl.ds(j, queries, stride=PITCH), :
                ].astype(jnp.bfloat16)

        part = pl.ds(c * ROWS, ROWS)
        outs.append(pltpu.make_async_copy(packed.at[part], returned.at[part], out_sem.at[c]))
        outs[-1].start()
    for copy in outs:
        copy.wait()
    sent = list(tables.values()) + [c for b in order for c in lat_copies[b]] + lon_copies
    for copy in sent + list(mix_copies.values()) + list(backs.values()):
        copy.wait_send()


def forward_rows(transform, field_v, wide, b):
    queries = transform.shape[0]

    @pl.loop(0, ROWS, unroll=4)
    def _(j):
        y = dot(transform, field_v[b * ROWS + j])
        for h in range(wide.shape[0]):
            wide.at[h][pl.ds(j, queries, stride=PITCH), :] = y[:, h * LANES : (h + 1) * LANES]


def relay_rows(wide, outgoing, b, lat_n, lon_n, per):
    @pl.loop(0, lat_n * lon_n)
    def _(d):
        a = d // lon_n
        k = lax.rem(d, lon_n)
        for i in range(per // 2):
            base = pl.multiple_of((d * (per // 2) + i) * (2 * PITCH), 8)
            for h in range(wide.shape[0]):
                both = wide[h, pl.ds(base, 2 * PITCH), :]
                for u in range(2):
                    outgoing[
                        a, k, 2 * i + u, b * ROWS : (b + 1) * ROWS, h * LANES : (h + 1) * LANES
                    ] = both[u * PITCH : u * PITCH + ROWS].astype(jnp.bfloat16)


def gelu(x):
    return 0.5 * x * (1.0 + lax.erf(x * math.sqrt(0.5)))


def grid_kernel(field, returned, table_t, skip, out, wide):
    rows, points, channels = field.shape
    queries = returned.shape[0]
    halves = channels // LANES

    @pl.loop(0, queries // 2)
    def _(i):
        base = pl.multiple_of(i * (2 * PITCH), 8)
        for u in range(2):
            row = returned[2 * i + u].astype(jnp.float32)
            for h in range(halves):
                wide[h, pl.ds(base + u * PITCH, ROWS), :] = row[:, h * LANES : (h + 1) * LANES]

    transform = table_t[...]
    weights = skip[...]

    @pl.loop(0, ROWS, unroll=2)
    def _(j):
        parts = [wide.at[h][pl.ds(j, queries, stride=PITCH), :] for h in range(halves)]
        values = jnp.concatenate(parts, axis=1).astype(jnp.bfloat16)
        spectral = dot(transform, values).astype(jnp.bfloat16).astype(jnp.float32)
        state = field[j]
        pre = spectral + dot(state, weights)
        out[j] = (state.astype(jnp.float32) + gelu(pre)).astype(jnp.bfloat16)


def packed_grid_kernel(field, returned, table, skip, mixed, out, spectrum, table_t):
    rows, points, channels = field.shape

    @pl.when(pl.program_id(0) == 0)
    def _():
        table_t[...] = table[...].astype(jnp.float32).T.astype(jnp.bfloat16)
        for s in range(mixed.shape[0]):
            both = mixed[s].astype(jnp.float32)
            spectrum[s] = jnp.stack([both[:, :channels], both[:, channels:]], axis=1).astype(jnp.bfloat16)

    transform = table_t[...]
    weights = skip[...]

    @pl.loop(0, rows, unroll=4)
    def _(j):
        spectral = dot(transform, returned[j]).astype(jnp.bfloat16).astype(jnp.float32)
        state = field[j]
        pre = spectral + dot(state, weights)
        out[j] = (state.astype(jnp.float32) + gelu(pre)).astype(jnp.bfloat16)


def per_device(lat_n, lon_n, field, mode_table, analysis, synthesis, mixing, degree_gain, skip_weight):
    rows, points, channels = field.shape
    modes = mode_table.shape[0]
    slots, degrees, all_rows = analysis.shape
    peers = lat_n * lon_n - 1
    queries = 2 * modes
    table = fourier_table(mode_table, lax.axis_index("lon") * points, points, points * lon_n)
    vmem = pl.BlockSpec(memory_space=pltpu.VMEM)
    anywhere = pl.BlockSpec(memory_space=pl.ANY)
    halves = channels // LANES
    wide_shape = (halves, queries * PITCH, LANES)
    blocks = rows // ROWS
    exchanged = (lat_n, lon_n, 2 * slots, rows, channels)
    coded = (lon_n, slots, degrees, 2 * channels)
    weights = (lon_n,) + analysis.shape
    staged = [
        ((rows, points, channels), jnp.bfloat16),
        (exchanged, jnp.bfloat16),
        ((lon_n, 2 * slots, lat_n, rows, channels), jnp.bfloat16),
        (weights, jnp.bfloat16),
        (weights, jnp.bfloat16),
        (coded, jnp.bfloat16),
        (coded, jnp.bfloat16),
        (coded, jnp.bfloat16),
        (exchanged, jnp.bfloat16),
        ((lon_n, lat_n, 2 * slots, rows, channels), jnp.bfloat16),
        ((rows, queries, channels), jnp.bfloat16),
    ]
    held = sum(2 * math.prod(shape) for shape, _ in staged) + 4 * blocks * math.prod(wide_shape)
    fits = held < VMEM_BYTES * 3 // 4
    dma = pltpu.SemaphoreType.DMA
    if fits:
        kernel = staged_kernel
        buffers = [pltpu.VMEM(shape, dtype) for shape, dtype in staged]
        scratch = [buffers[0], pltpu.VMEM((blocks * halves,) + wide_shape[1:], jnp.float32)] + buffers[1:] + [
            dma((rows // ROWS,)),
            dma((lon_n,)),
            dma((2, lon_n)),
            dma((2, lon_n)),
            dma((blocks, lon_n, lat_n)),
            dma((blocks, lon_n, lat_n)),
            dma((lon_n,)),
            dma((lon_n,)),
            dma((lon_n,)),
            dma((lon_n,)),
            dma((lon_n, lat_n)),
            dma((lon_n, lat_n)),
            dma((blocks,)),
        ]
    else:
        kernel = spectral_kernel
        scratch = [
            pltpu.VMEM((rows, points, channels), jnp.bfloat16),
            pltpu.VMEM(wide_shape, jnp.float32),
            pltpu.VMEM((queries, rows, channels), jnp.bfloat16),
            pltpu.VMEM((2 * slots, peers + 1, rows, channels), jnp.bfloat16),
            pltpu.VMEM((2 * slots, lat_n, rows, channels), jnp.bfloat16),
            dma((rows // ROWS,)),
            dma,
        ] + [dma((peers,))] * 4
    mixed, returned = pl.pallas_call(
        functools.partial(kernel, lat_n, lon_n),
        out_shape=(
            jax.ShapeDtypeStruct((slots, degrees, 2 * channels), jnp.bfloat16),
            jax.ShapeDtypeStruct((rows, queries, channels) if fits else (queries, rows, channels), jnp.bfloat16),
        ),
        in_specs=[anywhere] + [vmem] * 5,
        out_specs=(vmem, anywhere),
        scratch_shapes=scratch,
        compiler_params=pltpu.CompilerParams(
            collective_id=0, has_side_effects=True, vmem_limit_bytes=VMEM_BYTES
        ),
    )(field, table, analysis, synthesis, mixing[0], degree_gain[0])
    if fits:
        step = ROWS // 2
        whole = lambda shape: pl.BlockSpec(shape, lambda i: (0,) * len(shape))
        spectrum = (slots, degrees, 2, channels)
        return pl.pallas_call(
            packed_grid_kernel,
            grid=(rows // step,),
            out_shape=(
                jax.ShapeDtypeStruct(field.shape, jnp.bfloat16),
                jax.ShapeDtypeStruct(spectrum, jnp.bfloat16),
            ),
            in_specs=[
                pl.BlockSpec((step, points, channels), lambda i: (i, 0, 0)),
                pl.BlockSpec((step, queries, channels), lambda i: (i, 0, 0)),
                whole(table.shape),
                whole((channels, channels)),
                whole(mixed.shape),
            ],
            out_specs=(pl.BlockSpec((step, points, channels), lambda i: (i, 0, 0)), whole(spectrum)),
            scratch_shapes=[pltpu.VMEM((points, queries), jnp.bfloat16)],
            compiler_params=pltpu.CompilerParams(vmem_limit_bytes=VMEM_BYTES),
        )(field, returned, table, skip_weight[0], mixed)
    advanced = pl.pallas_call(
        grid_kernel,
        grid=(rows // ROWS,),
        out_shape=jax.ShapeDtypeStruct(field.shape, jnp.bfloat16),
        in_specs=[
            pl.BlockSpec((ROWS, points, channels), lambda i: (i, 0, 0)),
            pl.BlockSpec((queries, ROWS, channels), lambda i: (0, i, 0)),
            pl.BlockSpec((points, queries), lambda i: (0, 0)),
            pl.BlockSpec((channels, channels), lambda i: (0, 0)),
        ],
        out_specs=pl.BlockSpec((ROWS, points, channels), lambda i: (i, 0, 0)),
        scratch_shapes=[pltpu.VMEM(wide_shape, jnp.float32)],
        compiler_params=pltpu.CompilerParams(vmem_limit_bytes=VMEM_BYTES),
    )(field, returned, table.T, skip_weight[0])
    return advanced, mixed.reshape(slots, degrees, 2, channels)


def solution(mesh):
    in_specs = (
        P(("member", "lat"), "lon", None),
        P(),
        P(("lat", "lon"), None, None),
        P(("lat", "lon"), None, None),
        P(),
        P(),
        P(),
    )
    out_specs = (P(("member", "lat"), "lon", None), P(("member", "lat", "lon"), None, None, None))
    body = functools.partial(per_device, mesh.shape["lat"], mesh.shape["lon"])
    return jax.shard_map(body, mesh=mesh, in_specs=in_specs, out_specs=out_specs, check_vma=False)
```

```python
import functools
import math

import jax
import jax.numpy as jnp
from jax import lax
from jax.experimental import pallas as pl
from jax.experimental.pallas import tpu as pltpu
from jax.sharding import PartitionSpec as P

ROWS = 16
PITCH = 20
LANES = 128
VMEM_BYTES = 60 * 1024 * 1024


def fourier_table(orders, first, count, length):
    points = first + jnp.arange(count, dtype=jnp.int32)
    if length % 4:
        angles = (orders[:, None] * points[None, :] % length).astype(jnp.float32) * (2.0 * math.pi / length)
        both = jnp.stack([jnp.cos(angles), -jnp.sin(angles)], axis=1)
        return both.reshape(2 * orders.shape[0], count).astype(jnp.bfloat16)
    quarter = (jnp.arange(2 * orders.shape[0], dtype=jnp.int32) % 2) * (length // 4)
    phases = (jnp.repeat(orders, 2)[:, None] * points[None, :] + quarter[:, None]) % length
    return jnp.cos(phases.astype(jnp.float32) * (2.0 * math.pi / length)).astype(jnp.bfloat16)


def dot(a, b):
    return jnp.dot(a, b, preferred_element_type=jnp.float32)


def dot_t(a, b):
    return lax.dot_general(a, b, (((0,), (0,)), ((), ())), preferred_element_type=jnp.float32)


def spectral_kernel(
    lat_n, lon_n,
    field, table, analysis, synthesis, mixing, gain,
    mixed, returned,
    field_v, wide, outgoing, incoming, made, load_sem, own_sem, send_sem, recv_sem, back_send, back_recv,
):
    lat = lax.axis_index("lat")
    lon = lax.axis_index("lon")
    me = lat * lon_n + lon
    rows, points, channels = field_v.shape
    slots, degrees, _ = analysis.shape
    per = 2 * slots
    offsets = [(a, b) for b in range(lon_n) for a in range(lat_n) if a or b]
    halves = channels // LANES
    blocks = rows // ROWS
    queries = table.shape[0]

    loads = []
    for b in range(blocks):
        part = pl.ds(b * ROWS, ROWS)
        load = pltpu.make_async_copy(field.at[part], field_v.at[part], load_sem.at[b])
        load.start()
        loads.append(load)
    barrier = pltpu.get_barrier_semaphore()

    def peer(a, b):
        return lax.rem(lat + a, lat_n), lax.rem(lon + b, lon_n)

    for a, b in offsets:
        to_lat, to_lon = peer(a, b)
        pl.semaphore_signal(
            barrier, inc=1, device_id={"lat": to_lat, "lon": to_lon}, device_id_type=pl.DeviceIdType.MESH
        )

    transform = table[...]
    for b in range(blocks):
        loads[b].wait()

        @pl.loop(0, ROWS)
        def _(j):
            y = dot(transform, field_v[b * ROWS + j])
            for h in range(halves):
                wide.at[h][pl.ds(j, queries, stride=PITCH), :] = y[:, h * LANES : (h + 1) * LANES]

        @pl.loop(0, queries // 2)
        def _(i):
            base = pl.multiple_of(i * (2 * PITCH), 8)
            for h in range(halves):
                both = wide[h, pl.ds(base, 2 * PITCH), :]
                for u in range(2):
                    outgoing[2 * i + u, b * ROWS : (b + 1) * ROWS, h * LANES : (h + 1) * LANES] = both[
                        u * PITCH : u * PITCH + ROWS
                    ].astype(jnp.bfloat16)

    pl.semaphore_wait(barrier, len(offsets))
    place = lon * lat_n + lat
    sends = []
    for n, (a, b) in enumerate(offsets):
        to_lat, to_lon = peer(a, b)
        copy = pltpu.make_async_remote_copy(
            src_ref=outgoing.at[pl.ds((to_lat * lon_n + to_lon) * per, per)],
            dst_ref=incoming.at[:, place],
            send_sem=send_sem.at[n],
            recv_sem=recv_sem.at[n],
            device_id={"lat": to_lat, "lon": to_lon},
            device_id_type=pl.DeviceIdType.MESH,
        )
        copy.start()
        sends.append(copy)
    own = pltpu.make_async_copy(outgoing.at[pl.ds(me * per, per)], incoming.at[:, place], own_sem)
    own.start()
    own.wait()
    for copy in sends:
        copy.wait_recv()

    real_w = mixing[0]
    imag_w = mixing[1]
    gains = gain[...]
    all_rows = lat_n * rows
    for s in range(slots):
        weights = analysis[s]
        parts = []
        for r in range(2):
            acc = None
            for b in range(lon_n):
                lat_data = incoming[2 * s + r, b * lat_n : (b + 1) * lat_n].reshape(all_rows, channels)
                term = dot(weights, lat_data)
                acc = term if acc is None else acc + term
            parts.append(acc.astype(jnp.bfloat16))
        real = (dot(parts[0], real_w) - dot(parts[1], imag_w)) * gains
        imag = (dot(parts[0], imag_w) + dot(parts[1], real_w)) * gains
        both = [real.astype(jnp.bfloat16), imag.astype(jnp.bfloat16)]
        for r in range(2):
            mixed[s, :, r * channels : (r + 1) * channels] = both[r]
            made[2 * s + r] = (
                dot_t(synthesis[s], both[r]).astype(jnp.bfloat16).reshape(lat_n, rows, channels)
            )

    backs = []
    spot = pl.ds(me * per, per)
    for n, (a, b) in enumerate(offsets):
        to_lat, to_lon = peer(a, b)
        copy = pltpu.make_async_remote_copy(
            src_ref=made.at[:, to_lat],
            dst_ref=returned.at[spot],
            send_sem=back_send.at[n],
            recv_sem=back_recv.at[n],
            device_id={"lat": to_lat, "lon": to_lon},
            device_id_type=pl.DeviceIdType.MESH,
        )
        copy.start()
        backs.append(copy)
    own = pltpu.make_async_copy(made.at[:, lat], returned.at[spot], own_sem)
    own.start()
    own.wait()
    for copy in sends:
        copy.wait_send()
    for copy in backs:
        copy.wait()


def staged_kernel(
    lat_n, lon_n,
    field, table, analysis, synthesis, mixing, gain,
    mixed, returned,
    field_v, wide, outgoing, gathered, analysis_all, synthesis_all, part_out, part_in, mixed_all, made, landing, packed,
    load_sem, own_sem, table_send, table_recv, lat_send, lat_recv, lon_send, lon_recv,
    mix_send, mix_recv, back_send, back_recv, out_sem,
):
    lat = lax.axis_index("lat")
    lon = lax.axis_index("lon")
    rows, points, channels = field_v.shape
    slots, degrees, _ = analysis.shape
    per = 2 * slots
    all_rows = lat_n * rows
    order = sorted(range(1, lon_n), key=lambda k: abs(2 * k - lon_n)) + [0]
    blocks = rows // ROWS
    halves = channels // LANES
    early = order[: lon_n // 2] if blocks > 1 else []

    def at_lat(a):
        return lax.rem(lat + a, lat_n)

    def at_lon(b):
        return lax.rem(lon + b + lon_n, lon_n)

    def remote(src, dst, send, recv, to_lat, to_lon):
        copy = pltpu.make_async_remote_copy(
            src_ref=src, dst_ref=dst, send_sem=send, recv_sem=recv,
            device_id={"lat": to_lat, "lon": to_lon}, device_id_type=pl.DeviceIdType.MESH,
        )
        copy.start()
        return copy

    loads = []
    for b in range(rows // ROWS):
        part = pl.ds(b * ROWS, ROWS)
        load = pltpu.make_async_copy(field.at[part], field_v.at[part], load_sem.at[b])
        load.start()
        loads.append(load)
    barrier = pltpu.get_barrier_semaphore()
    peers = [(at_lat(a), lon) for a in range(1, lat_n)] + [(lat, at_lon(b)) for b in range(1, lon_n)]
    for to_lat, to_lon in peers:
        pl.semaphore_signal(
            barrier, inc=1, device_id={"lat": to_lat, "lon": to_lon}, device_id_type=pl.DeviceIdType.MESH
        )

    def to_owners(b, part, index):
        target = at_lon(b)
        return [
            remote(
                outgoing.at[at_lat(a), target, :, part], gathered.at[b, :, lat, part],
                lat_send.at[index, b, a], lat_recv.at[index, b, a], at_lat(a), lon,
            )
            for a in range(1, lat_n)
        ]

    tables = {}
    lat_copies = {b: [] for b in order}
    transform = table[...]
    for b in range(blocks):
        loads[b].wait()
        slabs = wide.at[pl.ds(b * halves, halves)]
        forward_rows(transform, field_v, slabs, b)
        relay_rows(slabs, outgoing, b, lat_n, lon_n, per)
        if b == 0:
            pl.semaphore_wait(barrier, len(peers))
        for k in early:
            lat_copies[k] += to_owners(k, pl.ds(b * ROWS, ROWS), b)
        if b == 0:
            for t, (src, dst) in enumerate(((analysis, analysis_all), (synthesis, synthesis_all))):
                for k in order[:-1]:
                    tables[t, k] = remote(
                        src, dst.at[k], table_send.at[t, k], table_recv.at[t, k], lat, at_lon(-k)
                    )
    owns = {}
    for b in order:
        if b not in early:
            lat_copies[b] += to_owners(b, pl.ds(0, rows), 0)
        owns[b] = pltpu.make_async_copy(outgoing.at[lat, at_lon(b)], gathered.at[b, :, lat], own_sem.at[b])
        owns[b].start()

    lon_copies = []
    kept = []
    for b in order:
        owns[b].wait()
        for copy in lat_copies[b]:
            copy.wait_recv()
        if b:
            tables[0, b].wait_recv()
        for s in range(slots):
            weights = analysis_all[b, s] if b else analysis[s]
            for r in range(2):
                value = dot(weights, gathered[b, 2 * s + r].reshape(all_rows, channels))
                if b:
                    part_out[b, s, :, r * channels : (r + 1) * channels] = value.astype(jnp.bfloat16)
                else:
                    kept.append(value)
        if b:
            lon_copies.append(
                remote(part_out.at[b], part_in.at[b], lon_send.at[b], lon_recv.at[b], lat, at_lon(b))
            )
    for copy in lon_copies:
        copy.wait_recv()

    real_w = mixing[0]
    imag_w = mixing[1]
    gains = gain[...]
    for s in range(slots):
        parts = []
        for r in range(2):
            total = kept[2 * s + r]
            for b in range(1, lon_n):
                total = total + part_in[b, s, :, r * channels : (r + 1) * channels].astype(jnp.float32)
            parts.append(total.astype(jnp.bfloat16))
        real = (dot(parts[0], real_w) - dot(parts[1], imag_w)) * gains
        imag = (dot(parts[0], imag_w) + dot(parts[1], real_w)) * gains
        mixed[s, :, :channels] = real.astype(jnp.bfloat16)
        mixed[s, :, channels:] = imag.astype(jnp.bfloat16)

    def mix_copy(src, k, send, to_lon):
        return pltpu.make_async_remote_copy(
            src_ref=src, dst_ref=mixed_all.at[k], send_sem=mix_send.at[send], recv_sem=mix_recv.at[k],
            device_id={"lat": lat, "lon": to_lon}, device_id_type=pl.DeviceIdType.MESH,
        )

    def onward(k, step):
        if k == 0:
            return mix_copy(mixed, 1 if step < 0 else lon_n - 1, 0 if step < 0 else lon_n, at_lon(step))
        return mix_copy(mixed_all.at[k], k - step, k, at_lon(step))

    def back_copy(k, a):
        return pltpu.make_async_remote_copy(
            src_ref=made.at[at_lat(a), k], dst_ref=landing.at[k, a],
            send_sem=back_send.at[k, a], recv_sem=back_recv.at[k, a],
            device_id={"lat": at_lat(a), "lon": lon}, device_id_type=pl.DeviceIdType.MESH,
        )

    def own_copy(k):
        return pltpu.make_async_copy(made.at[lat, k], landing.at[k, 0], own_sem.at[k])

    def emit(k):
        for s in range(slots):
            weights = synthesis_all[k, s] if k else synthesis[s]
            values = dot_t(weights, mixed_all[k, s] if k else mixed[s]).astype(jnp.bfloat16)
            for r in range(2):
                for a in range(lat_n):
                    made[a, k, 2 * s + r] = values[a * rows : (a + 1) * rows, r * channels : (r + 1) * channels]
        for a in range(1, lat_n):
            back_copy(k, a).start()
        own_copy(k).start()

    has_right = lon < lon_n - 1
    has_left = lon > 0

    @pl.when(has_right)
    def _():
        onward(0, 1).start()

    @pl.when(has_left)
    def _():
        onward(0, -1).start()

    emit(0)
    for k in order[:-1]:
        tables[1, k].wait_recv()
    for d in range(1, lon_n):

        @pl.when(lon >= d)
        def _():
            mix_copy(mixed, lon_n - d, lon_n - d, at_lon(1)).wait_recv()
            if d < lon_n - 1:

                @pl.when(has_right)
                def _():
                    onward(lon_n - d, 1).start()

            emit(lon_n - d)

        @pl.when(lon + d < lon_n)
        def _():
            mix_copy(mixed, d, d, at_lon(1)).wait_recv()
            if d < lon_n - 1:

                @pl.when(has_left)
                def _():
                    onward(d, -1).start()

            emit(d)

    back_order = [0] + sorted(range(1, lon_n), key=lambda k: -abs(2 * k - lon_n))
    for b in back_order:
        own_copy(b).wait()
        for a in range(1, lat_n):
            back_copy(b, a).wait_recv()
        for a in range(lat_n):
            source = at_lat(lat_n - a) * lon_n + at_lon(b)
            base = pl.multiple_of(source * (per * PITCH), 8)
            for i in range(per):
                values = landing[b, a, i].astype(jnp.float32)
                for c in range(blocks):
                    for h in range(halves):
                        wide[c * halves + h, pl.ds(base + i * PITCH, ROWS), :] = values[
                            c * ROWS : (c + 1) * ROWS, h * LANES : (h + 1) * LANES
                        ]

    queries = table.shape[0]
    outs = []
    for c in range(blocks):

        @pl.loop(0, ROWS, unroll=4)
        def _(j):
            for h in range(halves):
                packed[c * ROWS + j, :, h * LANES : (h + 1) * LANES] = wide.at[c * halves + h][
                    pl.ds(j, queries, stride=PITCH), :
                ].astype(jnp.bfloat16)

        part = pl.ds(c * ROWS, ROWS)
        outs.append(pltpu.make_async_copy(packed.at[part], returned.at[part], out_sem.at[c]))
        outs[-1].start()
    for copy in outs:
        copy.wait()
    sent = list(tables.values()) + [c for b in order for c in lat_copies[b]] + lon_copies
    for copy in sent + [back_copy(b, a) for b in range(lon_n) for a in range(1, lat_n)]:
        copy.wait_send()

    @pl.when(has_right)
    def _():
        onward(0, 1).wait_send()

    @pl.when(has_left)
    def _():
        onward(0, -1).wait_send()

    for d in range(1, lon_n - 1):

        @pl.when((lon >= d) & has_right)
        def _():
            onward(lon_n - d, 1).wait_send()

        @pl.when((lon + d < lon_n) & has_left)
        def _():
            onward(d, -1).wait_send()


def forward_rows(transform, field_v, wide, b):
    queries = transform.shape[0]

    @pl.loop(0, ROWS, unroll=4)
    def _(j):
        y = dot(transform, field_v[b * ROWS + j])
        for h in range(wide.shape[0]):
            wide.at[h][pl.ds(j, queries, stride=PITCH), :] = y[:, h * LANES : (h + 1) * LANES]


def relay_rows(wide, outgoing, b, lat_n, lon_n, per):
    @pl.loop(0, lat_n * lon_n)
    def _(d):
        a = d // lon_n
        k = lax.rem(d, lon_n)
        for i in range(per // 2):
            base = pl.multiple_of((d * (per // 2) + i) * (2 * PITCH), 8)
            for h in range(wide.shape[0]):
                both = wide[h, pl.ds(base, 2 * PITCH), :]
                for u in range(2):
                    outgoing[
                        a, k, 2 * i + u, b * ROWS : (b + 1) * ROWS, h * LANES : (h + 1) * LANES
                    ] = both[u * PITCH : u * PITCH + ROWS].astype(jnp.bfloat16)


def gelu(x):
    return 0.5 * x * (1.0 + lax.erf(x * math.sqrt(0.5)))


def grid_kernel(field, returned, table_t, skip, out, wide):
    rows, points, channels = field.shape
    queries = returned.shape[0]
    halves = channels // LANES

    @pl.loop(0, queries // 2)
    def _(i):
        base = pl.multiple_of(i * (2 * PITCH), 8)
        for u in range(2):
            row = returned[2 * i + u].astype(jnp.float32)
            for h in range(halves):
                wide[h, pl.ds(base + u * PITCH, ROWS), :] = row[:, h * LANES : (h + 1) * LANES]

    transform = table_t[...]
    weights = skip[...]

    @pl.loop(0, ROWS, unroll=2)
    def _(j):
        parts = [wide.at[h][pl.ds(j, queries, stride=PITCH), :] for h in range(halves)]
        values = jnp.concatenate(parts, axis=1).astype(jnp.bfloat16)
        spectral = dot(transform, values).astype(jnp.bfloat16).astype(jnp.float32)
        state = field[j]
        pre = spectral + dot(state, weights)
        out[j] = (state.astype(jnp.float32) + gelu(pre)).astype(jnp.bfloat16)


def packed_grid_kernel(field, returned, table, skip, mixed, out, spectrum, table_t):
    rows, points, channels = field.shape

    @pl.when(pl.program_id(0) == 0)
    def _():
        table_t[...] = table[...].astype(jnp.float32).T.astype(jnp.bfloat16)
        for s in range(mixed.shape[0]):
            both = mixed[s].astype(jnp.float32)
            spectrum[s] = jnp.stack([both[:, :channels], both[:, channels:]], axis=1).astype(jnp.bfloat16)

    transform = table_t[...]
    weights = skip[...]

    @pl.loop(0, rows, unroll=4)
    def _(j):
        spectral = dot(transform, returned[j]).astype(jnp.bfloat16).astype(jnp.float32)
        state = field[j]
        pre = spectral + dot(state, weights)
        out[j] = (state.astype(jnp.float32) + gelu(pre)).astype(jnp.bfloat16)


def per_device(lat_n, lon_n, field, mode_table, analysis, synthesis, mixing, degree_gain, skip_weight):
    rows, points, channels = field.shape
    modes = mode_table.shape[0]
    slots, degrees, all_rows = analysis.shape
    peers = lat_n * lon_n - 1
    queries = 2 * modes
    table = fourier_table(mode_table, lax.axis_index("lon") * points, points, points * lon_n)
    vmem = pl.BlockSpec(memory_space=pltpu.VMEM)
    anywhere = pl.BlockSpec(memory_space=pl.ANY)
    halves = channels // LANES
    wide_shape = (halves, queries * PITCH, LANES)
    blocks = rows // ROWS
    exchanged = (lat_n, lon_n, 2 * slots, rows, channels)
    coded = (lon_n, slots, degrees, 2 * channels)
    weights = (lon_n,) + analysis.shape
    staged = [
        ((rows, points, channels), jnp.bfloat16),
        (exchanged, jnp.bfloat16),
        ((lon_n, 2 * slots, lat_n, rows, channels), jnp.bfloat16),
        (weights, jnp.bfloat16),
        (weights, jnp.bfloat16),
        (coded, jnp.bfloat16),
        (coded, jnp.bfloat16),
        (coded, jnp.bfloat16),
        (exchanged, jnp.bfloat16),
        ((lon_n, lat_n, 2 * slots, rows, channels), jnp.bfloat16),
        ((rows, queries, channels), jnp.bfloat16),
    ]
    held = sum(2 * math.prod(shape) for shape, _ in staged) + 4 * blocks * math.prod(wide_shape)
    fits = held < VMEM_BYTES * 3 // 4
    dma = pltpu.SemaphoreType.DMA
    if fits:
        kernel = staged_kernel
        buffers = [pltpu.VMEM(shape, dtype) for shape, dtype in staged]
        scratch = [buffers[0], pltpu.VMEM((blocks * halves,) + wide_shape[1:], jnp.float32)] + buffers[1:] + [
            dma((rows // ROWS,)),
            dma((lon_n,)),
            dma((2, lon_n)),
            dma((2, lon_n)),
            dma((blocks, lon_n, lat_n)),
            dma((blocks, lon_n, lat_n)),
            dma((lon_n,)),
            dma((lon_n,)),
            dma((lon_n + 1,)),
            dma((lon_n,)),
            dma((lon_n, lat_n)),
            dma((lon_n, lat_n)),
            dma((blocks,)),
        ]
    else:
        kernel = spectral_kernel
        scratch = [
            pltpu.VMEM((rows, points, channels), jnp.bfloat16),
            pltpu.VMEM(wide_shape, jnp.float32),
            pltpu.VMEM((queries, rows, channels), jnp.bfloat16),
            pltpu.VMEM((2 * slots, peers + 1, rows, channels), jnp.bfloat16),
            pltpu.VMEM((2 * slots, lat_n, rows, channels), jnp.bfloat16),
            dma((rows // ROWS,)),
            dma,
        ] + [dma((peers,))] * 4
    mixed, returned = pl.pallas_call(
        functools.partial(kernel, lat_n, lon_n),
        out_shape=(
            jax.ShapeDtypeStruct((slots, degrees, 2 * channels), jnp.bfloat16),
            jax.ShapeDtypeStruct((rows, queries, channels) if fits else (queries, rows, channels), jnp.bfloat16),
        ),
        in_specs=[anywhere] + [vmem] * 5,
        out_specs=(vmem, anywhere),
        scratch_shapes=scratch,
        compiler_params=pltpu.CompilerParams(
            collective_id=0, has_side_effects=True, vmem_limit_bytes=VMEM_BYTES
        ),
    )(field, table, analysis, synthesis, mixing[0], degree_gain[0])
    if fits:
        step = ROWS // 2
        whole = lambda shape: pl.BlockSpec(shape, lambda i: (0,) * len(shape))
        spectrum = (slots, degrees, 2, channels)
        return pl.pallas_call(
            packed_grid_kernel,
            grid=(rows // step,),
            out_shape=(
                jax.ShapeDtypeStruct(field.shape, jnp.bfloat16),
                jax.ShapeDtypeStruct(spectrum, jnp.bfloat16),
            ),
            in_specs=[
                pl.BlockSpec((step, points, channels), lambda i: (i, 0, 0)),
                pl.BlockSpec((step, queries, channels), lambda i: (i, 0, 0)),
                whole(table.shape),
                whole((channels, channels)),
                whole(mixed.shape),
            ],
            out_specs=(pl.BlockSpec((step, points, channels), lambda i: (i, 0, 0)), whole(spectrum)),
            scratch_shapes=[pltpu.VMEM((points, queries), jnp.bfloat16)],
            compiler_params=pltpu.CompilerParams(vmem_limit_bytes=VMEM_BYTES),
        )(field, returned, table, skip_weight[0], mixed)
    advanced = pl.pallas_call(
        grid_kernel,
        grid=(rows // ROWS,),
        out_shape=jax.ShapeDtypeStruct(field.shape, jnp.bfloat16),
        in_specs=[
            pl.BlockSpec((ROWS, points, channels), lambda i: (i, 0, 0)),
            pl.BlockSpec((queries, ROWS, channels), lambda i: (0, i, 0)),
            pl.BlockSpec((points, queries), lambda i: (0, 0)),
            pl.BlockSpec((channels, channels), lambda i: (0, 0)),
        ],
        out_specs=pl.BlockSpec((ROWS, points, channels), lambda i: (i, 0, 0)),
        scratch_shapes=[pltpu.VMEM(wide_shape, jnp.float32)],
        compiler_params=pltpu.CompilerParams(vmem_limit_bytes=VMEM_BYTES),
    )(field, returned, table.T, skip_weight[0])
    return advanced, mixed.reshape(slots, degrees, 2, channels)


def solution(mesh):
    in_specs = (
        P(("member", "lat"), "lon", None),
        P(),
        P(("lat", "lon"), None, None),
        P(("lat", "lon"), None, None),
        P(),
        P(),
        P(),
    )
    out_specs = (P(("member", "lat"), "lon", None), P(("member", "lat", "lon"), None, None, None))
    body = functools.partial(per_device, mesh.shape["lat"], mesh.shape["lon"])
    return jax.shard_map(body, mesh=mesh, in_specs=in_specs, out_specs=out_specs, check_vma=False)
```

```python
import functools
import math

import jax
import jax.numpy as jnp
from jax import lax
from jax.experimental import pallas as pl
from jax.experimental.pallas import tpu as pltpu
from jax.sharding import PartitionSpec as P

ROWS = 16
PITCH = 20
LANES = 128
VMEM_BYTES = 60 * 1024 * 1024


def fourier_table(orders, first, count, length):
    points = first + jnp.arange(count, dtype=jnp.int32)
    phases = orders[:, None] * points[None, :] % length
    angles = phases.astype(jnp.float32) * (2.0 * math.pi / length)
    return (
        jnp.stack([jnp.cos(angles), -jnp.sin(angles)], axis=1)
        .reshape(2 * orders.shape[0], count)
        .astype(jnp.bfloat16)
    )


def dot(a, b):
    return jnp.dot(a, b, preferred_element_type=jnp.float32)


def dot_t(a, b):
    return lax.dot_general(a, b, (((0,), (0,)), ((), ())), preferred_element_type=jnp.float32)


def spectral_kernel(
    lat_n, lon_n,
    field, table, analysis, synthesis, mixing, gain,
    mixed, returned,
    field_v, wide, outgoing, incoming, made, load_sem, own_sem, send_sem, recv_sem, back_send, back_recv,
):
    lat = lax.axis_index("lat")
    lon = lax.axis_index("lon")
    me = lat * lon_n + lon
    rows, points, channels = field_v.shape
    slots, degrees, _ = analysis.shape
    per = 2 * slots
    offsets = [(a, b) for b in range(lon_n) for a in range(lat_n) if a or b]
    halves = channels // LANES
    blocks = rows // ROWS
    queries = table.shape[0]

    loads = []
    for b in range(blocks):
        part = pl.ds(b * ROWS, ROWS)
        load = pltpu.make_async_copy(field.at[part], field_v.at[part], load_sem.at[b])
        load.start()
        loads.append(load)
    barrier = pltpu.get_barrier_semaphore()

    def peer(a, b):
        return lax.rem(lat + a, lat_n), lax.rem(lon + b, lon_n)

    for a, b in offsets:
        to_lat, to_lon = peer(a, b)
        pl.semaphore_signal(
            barrier, inc=1, device_id={"lat": to_lat, "lon": to_lon}, device_id_type=pl.DeviceIdType.MESH
        )

    transform = table[...]
    for b in range(blocks):
        loads[b].wait()

        @pl.loop(0, ROWS)
        def _(j):
            y = dot(transform, field_v[b * ROWS + j])
            for h in range(halves):
                wide.at[h][pl.ds(j, queries, stride=PITCH), :] = y[:, h * LANES : (h + 1) * LANES]

        @pl.loop(0, queries // 2)
        def _(i):
            base = pl.multiple_of(i * (2 * PITCH), 8)
            for h in range(halves):
                both = wide[h, pl.ds(base, 2 * PITCH), :]
                for u in range(2):
                    outgoing[2 * i + u, b * ROWS : (b + 1) * ROWS, h * LANES : (h + 1) * LANES] = both[
                        u * PITCH : u * PITCH + ROWS
                    ].astype(jnp.bfloat16)

    pl.semaphore_wait(barrier, len(offsets))
    place = lon * lat_n + lat
    sends = []
    for n, (a, b) in enumerate(offsets):
        to_lat, to_lon = peer(a, b)
        copy = pltpu.make_async_remote_copy(
            src_ref=outgoing.at[pl.ds((to_lat * lon_n + to_lon) * per, per)],
            dst_ref=incoming.at[:, place],
            send_sem=send_sem.at[n],
            recv_sem=recv_sem.at[n],
            device_id={"lat": to_lat, "lon": to_lon},
            device_id_type=pl.DeviceIdType.MESH,
        )
        copy.start()
        sends.append(copy)
    own = pltpu.make_async_copy(outgoing.at[pl.ds(me * per, per)], incoming.at[:, place], own_sem)
    own.start()
    own.wait()
    for copy in sends:
        copy.wait_recv()

    real_w = mixing[0]
    imag_w = mixing[1]
    gains = gain[...]
    all_rows = lat_n * rows
    for s in range(slots):
        weights = analysis[s]
        parts = []
        for r in range(2):
            acc = None
            for b in range(lon_n):
                lat_data = incoming[2 * s + r, b * lat_n : (b + 1) * lat_n].reshape(all_rows, channels)
                term = dot(weights, lat_data)
                acc = term if acc is None else acc + term
            parts.append(acc.astype(jnp.bfloat16))
        real = (dot(parts[0], real_w) - dot(parts[1], imag_w)) * gains
        imag = (dot(parts[0], imag_w) + dot(parts[1], real_w)) * gains
        both = [real.astype(jnp.bfloat16), imag.astype(jnp.bfloat16)]
        for r in range(2):
            mixed[s, :, r * channels : (r + 1) * channels] = both[r]
            made[2 * s + r] = (
                dot_t(synthesis[s], both[r]).astype(jnp.bfloat16).reshape(lat_n, rows, channels)
            )

    backs = []
    spot = pl.ds(me * per, per)
    for n, (a, b) in enumerate(offsets):
        to_lat, to_lon = peer(a, b)
        copy = pltpu.make_async_remote_copy(
            src_ref=made.at[:, to_lat],
            dst_ref=returned.at[spot],
            send_sem=back_send.at[n],
            recv_sem=back_recv.at[n],
            device_id={"lat": to_lat, "lon": to_lon},
            device_id_type=pl.DeviceIdType.MESH,
        )
        copy.start()
        backs.append(copy)
    own = pltpu.make_async_copy(made.at[:, lat], returned.at[spot], own_sem)
    own.start()
    own.wait()
    for copy in sends:
        copy.wait_send()
    for copy in backs:
        copy.wait()


def staged_kernel(
    lat_n, lon_n,
    field, table, analysis, synthesis, mixing, gain,
    mixed, returned,
    field_v, wide, outgoing, gathered, analysis_all, synthesis_all, part_out, part_in, mixed_all, made, landing, packed,
    load_sem, own_sem, table_send, table_recv, lat_send, lat_recv, lon_send, lon_recv,
    mix_send, mix_recv, back_send, back_recv, out_sem,
):
    lat = lax.axis_index("lat")
    lon = lax.axis_index("lon")
    rows, points, channels = field_v.shape
    slots, degrees, _ = analysis.shape
    per = 2 * slots
    all_rows = lat_n * rows
    order = sorted(range(1, lon_n), key=lambda k: abs(2 * k - lon_n)) + [0]
    blocks = rows // ROWS
    halves = channels // LANES
    early = order[: lon_n // 2] if blocks > 1 else []

    def at_lat(a):
        return lax.rem(lat + a, lat_n)

    def at_lon(b):
        return lax.rem(lon + b + lon_n, lon_n)

    def remote(src, dst, send, recv, to_lat, to_lon):
        copy = pltpu.make_async_remote_copy(
            src_ref=src, dst_ref=dst, send_sem=send, recv_sem=recv,
            device_id={"lat": to_lat, "lon": to_lon}, device_id_type=pl.DeviceIdType.MESH,
        )
        copy.start()
        return copy

    loads = []
    for b in range(rows // ROWS):
        part = pl.ds(b * ROWS, ROWS)
        load = pltpu.make_async_copy(field.at[part], field_v.at[part], load_sem.at[b])
        load.start()
        loads.append(load)
    barrier = pltpu.get_barrier_semaphore()
    peers = [(at_lat(a), lon) for a in range(1, lat_n)] + [(lat, at_lon(b)) for b in range(1, lon_n)]
    for to_lat, to_lon in peers:
        pl.semaphore_signal(
            barrier, inc=1, device_id={"lat": to_lat, "lon": to_lon}, device_id_type=pl.DeviceIdType.MESH
        )

    def to_owners(b, part, index):
        target = at_lon(b)
        return [
            remote(
                outgoing.at[at_lat(a), target, :, part], gathered.at[b, :, lat, part],
                lat_send.at[index, b, a], lat_recv.at[index, b, a], at_lat(a), lon,
            )
            for a in range(1, lat_n)
        ]

    tables = {}
    lat_copies = {b: [] for b in order}
    transform = table[...]
    for b in range(blocks):
        loads[b].wait()
        slabs = wide.at[pl.ds(b * halves, halves)]
        forward_rows(transform, field_v, slabs, b)
        relay_rows(slabs, outgoing, b, lat_n, lon_n, per)
        if b == 0:
            pl.semaphore_wait(barrier, len(peers))
        for k in early:
            lat_copies[k] += to_owners(k, pl.ds(b * ROWS, ROWS), b)
        if b == 0:
            for t, (src, dst) in enumerate(((analysis, analysis_all), (synthesis, synthesis_all))):
                for k in order[:-1]:
                    tables[t, k] = remote(
                        src, dst.at[k], table_send.at[t, k], table_recv.at[t, k], lat, at_lon(-k)
                    )
    owns = {}
    for b in order:
        if b not in early:
            lat_copies[b] += to_owners(b, pl.ds(0, rows), 0)
        owns[b] = pltpu.make_async_copy(outgoing.at[lat, at_lon(b)], gathered.at[b, :, lat], own_sem.at[b])
        owns[b].start()

    lon_copies = []
    kept = []
    for b in order:
        owns[b].wait()
        for copy in lat_copies[b]:
            copy.wait_recv()
        if b:
            tables[0, b].wait_recv()
        for s in range(slots):
            weights = analysis_all[b, s] if b else analysis[s]
            for r in range(2):
                value = dot(weights, gathered[b, 2 * s + r].reshape(all_rows, channels))
                if b:
                    part_out[b, s, :, r * channels : (r + 1) * channels] = value.astype(jnp.bfloat16)
                else:
                    kept.append(value)
        if b:
            lon_copies.append(
                remote(part_out.at[b], part_in.at[b], lon_send.at[b], lon_recv.at[b], lat, at_lon(b))
            )
    for copy in lon_copies:
        copy.wait_recv()

    real_w = mixing[0]
    imag_w = mixing[1]
    gains = gain[...]
    back_order = order[::-1]
    mix_copies = {}
    backs = {}

    def emit(b, s):
        weights = synthesis_all[b, s] if b else synthesis[s]
        values = dot_t(weights, mixed_all[b, s] if b else mixed[s]).astype(jnp.bfloat16)
        for r in range(2):
            for a in range(lat_n):
                made[a, b, 2 * s + r] = values[a * rows : (a + 1) * rows, r * channels : (r + 1) * channels]
        part = pl.ds(2 * s, 2)
        for a in range(1, lat_n):
            backs[b, s, a] = remote(
                made.at[at_lat(a), b, part], landing.at[b, a, part],
                back_send.at[b * slots + s, a], back_recv.at[b * slots + s, a], at_lat(a), lon,
            )

    for s in range(slots):
        parts = []
        for r in range(2):
            total = kept[2 * s + r]
            for b in range(1, lon_n):
                total = total + part_in[b, s, :, r * channels : (r + 1) * channels].astype(jnp.float32)
            parts.append(total.astype(jnp.bfloat16))
        real = (dot(parts[0], real_w) - dot(parts[1], imag_w)) * gains
        imag = (dot(parts[0], imag_w) + dot(parts[1], real_w)) * gains
        mixed[s, :, :channels] = real.astype(jnp.bfloat16)
        mixed[s, :, channels:] = imag.astype(jnp.bfloat16)
        for b in back_order[1:]:
            n = b * slots + s
            mix_copies[b, s] = remote(
                mixed.at[s], mixed_all.at[b, s], mix_send.at[n], mix_recv.at[n], lat, at_lon(-b)
            )
        emit(0, s)
    for b in back_order:
        if b:
            tables[1, b].wait_recv()
            for s in range(slots):
                mix_copies[b, s].wait_recv()
                emit(b, s)
        owns[b] = pltpu.make_async_copy(made.at[lat, b], landing.at[b, 0], own_sem.at[b])
        owns[b].start()

    for b in back_order:
        owns[b].wait()
        for a in range(1, lat_n):
            for s in range(slots):
                backs[b, s, a].wait_recv()
        for a in range(lat_n):
            source = at_lat(lat_n - a) * lon_n + at_lon(b)
            base = pl.multiple_of(source * (per * PITCH), 8)
            for i in range(per):
                values = landing[b, a, i].astype(jnp.float32)
                for c in range(blocks):
                    for h in range(halves):
                        wide[c * halves + h, pl.ds(base + i * PITCH, ROWS), :] = values[
                            c * ROWS : (c + 1) * ROWS, h * LANES : (h + 1) * LANES
                        ]

    queries = table.shape[0]
    outs = []
    for c in range(blocks):

        @pl.loop(0, ROWS, unroll=4)
        def _(j):
            for h in range(halves):
                packed[c * ROWS + j, :, h * LANES : (h + 1) * LANES] = wide.at[c * halves + h][
                    pl.ds(j, queries, stride=PITCH), :
                ].astype(jnp.bfloat16)

        part = pl.ds(c * ROWS, ROWS)
        outs.append(pltpu.make_async_copy(packed.at[part], returned.at[part], out_sem.at[c]))
        outs[-1].start()
    for copy in outs:
        copy.wait()
    sent = list(tables.values()) + [c for b in order for c in lat_copies[b]] + lon_copies
    for copy in sent + list(mix_copies.values()) + list(backs.values()):
        copy.wait_send()


def forward_rows(transform, field_v, wide, b):
    queries = transform.shape[0]

    @pl.loop(0, ROWS, unroll=4)
    def _(j):
        y = dot(transform, field_v[b * ROWS + j])
        for h in range(wide.shape[0]):
            wide.at[h][pl.ds(j, queries, stride=PITCH), :] = y[:, h * LANES : (h + 1) * LANES]


def relay_rows(wide, outgoing, b, lat_n, lon_n, per):
    @pl.loop(0, lat_n * lon_n)
    def _(d):
        a = d // lon_n
        k = lax.rem(d, lon_n)
        for i in range(per // 2):
            base = pl.multiple_of((d * (per // 2) + i) * (2 * PITCH), 8)
            for h in range(wide.shape[0]):
                both = wide[h, pl.ds(base, 2 * PITCH), :]
                for u in range(2):
                    outgoing[
                        a, k, 2 * i + u, b * ROWS : (b + 1) * ROWS, h * LANES : (h + 1) * LANES
                    ] = both[u * PITCH : u * PITCH + ROWS].astype(jnp.bfloat16)


def gelu(x):
    return 0.5 * x * (1.0 + lax.erf(x * math.sqrt(0.5)))


def grid_kernel(field, returned, table_t, skip, out, wide):
    rows, points, channels = field.shape
    queries = returned.shape[0]
    halves = channels // LANES

    @pl.loop(0, queries // 2)
    def _(i):
        base = pl.multiple_of(i * (2 * PITCH), 8)
        for u in range(2):
            row = returned[2 * i + u].astype(jnp.float32)
            for h in range(halves):
                wide[h, pl.ds(base + u * PITCH, ROWS), :] = row[:, h * LANES : (h + 1) * LANES]

    transform = table_t[...]
    weights = skip[...]

    @pl.loop(0, ROWS, unroll=2)
    def _(j):
        parts = [wide.at[h][pl.ds(j, queries, stride=PITCH), :] for h in range(halves)]
        values = jnp.concatenate(parts, axis=1).astype(jnp.bfloat16)
        spectral = dot(transform, values).astype(jnp.bfloat16).astype(jnp.float32)
        state = field[j]
        pre = spectral + dot(state, weights)
        out[j] = (state.astype(jnp.float32) + gelu(pre)).astype(jnp.bfloat16)


def packed_grid_kernel(field, returned, table, skip, mixed, out, spectrum, table_t):
    rows, points, channels = field.shape

    @pl.when(pl.program_id(0) == 0)
    def _():
        table_t[...] = table[...].astype(jnp.float32).T.astype(jnp.bfloat16)
        for s in range(mixed.shape[0]):
            both = mixed[s].astype(jnp.float32)
            spectrum[s] = jnp.stack([both[:, :channels], both[:, channels:]], axis=1).astype(jnp.bfloat16)

    transform = table_t[...]
    weights = skip[...]

    @pl.loop(0, rows, unroll=4)
    def _(j):
        spectral = dot(transform, returned[j]).astype(jnp.bfloat16).astype(jnp.float32)
        state = field[j]
        pre = spectral + dot(state, weights)
        out[j] = (state.astype(jnp.float32) + gelu(pre)).astype(jnp.bfloat16)


def per_device(lat_n, lon_n, field, mode_table, analysis, synthesis, mixing, degree_gain, skip_weight):
    rows, points, channels = field.shape
    modes = mode_table.shape[0]
    slots, degrees, all_rows = analysis.shape
    peers = lat_n * lon_n - 1
    queries = 2 * modes
    table = fourier_table(mode_table, lax.axis_index("lon") * points, points, points * lon_n)
    vmem = pl.BlockSpec(memory_space=pltpu.VMEM)
    anywhere = pl.BlockSpec(memory_space=pl.ANY)
    halves = channels // LANES
    wide_shape = (halves, queries * PITCH, LANES)
    blocks = rows // ROWS
    exchanged = (lat_n, lon_n, 2 * slots, rows, channels)
    coded = (lon_n, slots, degrees, 2 * channels)
    weights = (lon_n,) + analysis.shape
    staged = [
        ((rows, points, channels), jnp.bfloat16),
        (exchanged, jnp.bfloat16),
        ((lon_n, 2 * slots, lat_n, rows, channels), jnp.bfloat16),
        (weights, jnp.bfloat16),
        (weights, jnp.bfloat16),
        (coded, jnp.bfloat16),
        (coded, jnp.bfloat16),
        (coded, jnp.bfloat16),
        (exchanged, jnp.bfloat16),
        ((lon_n, lat_n, 2 * slots, rows, channels), jnp.bfloat16),
        ((rows, queries, channels), jnp.bfloat16),
    ]
    held = sum(2 * math.prod(shape) for shape, _ in staged) + 4 * blocks * math.prod(wide_shape)
    fits = held < VMEM_BYTES * 3 // 4
    dma = pltpu.SemaphoreType.DMA
    if fits:
        kernel = staged_kernel
        buffers = [pltpu.VMEM(shape, dtype) for shape, dtype in staged]
        scratch = [buffers[0], pltpu.VMEM((blocks * halves,) + wide_shape[1:], jnp.float32)] + buffers[1:] + [
            dma((rows // ROWS,)),
            dma((lon_n,)),
            dma((2, lon_n)),
            dma((2, lon_n)),
            dma((blocks, lon_n, lat_n)),
            dma((blocks, lon_n, lat_n)),
            dma((lon_n,)),
            dma((lon_n,)),
            dma((lon_n * slots,)),
            dma((lon_n * slots,)),
            dma((lon_n * slots, lat_n)),
            dma((lon_n * slots, lat_n)),
            dma((blocks,)),
        ]
    else:
        kernel = spectral_kernel
        scratch = [
            pltpu.VMEM((rows, points, channels), jnp.bfloat16),
            pltpu.VMEM(wide_shape, jnp.float32),
            pltpu.VMEM((queries, rows, channels), jnp.bfloat16),
            pltpu.VMEM((2 * slots, peers + 1, rows, channels), jnp.bfloat16),
            pltpu.VMEM((2 * slots, lat_n, rows, channels), jnp.bfloat16),
            dma((rows // ROWS,)),
            dma,
        ] + [dma((peers,))] * 4
    mixed, returned = pl.pallas_call(
        functools.partial(kernel, lat_n, lon_n),
        out_shape=(
            jax.ShapeDtypeStruct((slots, degrees, 2 * channels), jnp.bfloat16),
            jax.ShapeDtypeStruct((rows, queries, channels) if fits else (queries, rows, channels), jnp.bfloat16),
        ),
        in_specs=[anywhere] + [vmem] * 5,
        out_specs=(vmem, anywhere),
        scratch_shapes=scratch,
        compiler_params=pltpu.CompilerParams(
            collective_id=0, has_side_effects=True, vmem_limit_bytes=VMEM_BYTES
        ),
    )(field, table, analysis, synthesis, mixing[0], degree_gain[0])
    if fits:
        step = ROWS // 2
        whole = lambda shape: pl.BlockSpec(shape, lambda i: (0,) * len(shape))
        spectrum = (slots, degrees, 2, channels)
        return pl.pallas_call(
            packed_grid_kernel,
            grid=(rows // step,),
            out_shape=(
                jax.ShapeDtypeStruct(field.shape, jnp.bfloat16),
                jax.ShapeDtypeStruct(spectrum, jnp.bfloat16),
            ),
            in_specs=[
                pl.BlockSpec((step, points, channels), lambda i: (i, 0, 0)),
                pl.BlockSpec((step, queries, channels), lambda i: (i, 0, 0)),
                whole(table.shape),
                whole((channels, channels)),
                whole(mixed.shape),
            ],
            out_specs=(pl.BlockSpec((step, points, channels), lambda i: (i, 0, 0)), whole(spectrum)),
            scratch_shapes=[pltpu.VMEM((points, queries), jnp.bfloat16)],
            compiler_params=pltpu.CompilerParams(vmem_limit_bytes=VMEM_BYTES),
        )(field, returned, table, skip_weight[0], mixed)
    advanced = pl.pallas_call(
        grid_kernel,
        grid=(rows // ROWS,),
        out_shape=jax.ShapeDtypeStruct(field.shape, jnp.bfloat16),
        in_specs=[
            pl.BlockSpec((ROWS, points, channels), lambda i: (i, 0, 0)),
            pl.BlockSpec((queries, ROWS, channels), lambda i: (0, i, 0)),
            pl.BlockSpec((points, queries), lambda i: (0, 0)),
            pl.BlockSpec((channels, channels), lambda i: (0, 0)),
        ],
        out_specs=pl.BlockSpec((ROWS, points, channels), lambda i: (i, 0, 0)),
        scratch_shapes=[pltpu.VMEM(wide_shape, jnp.float32)],
        compiler_params=pltpu.CompilerParams(vmem_limit_bytes=VMEM_BYTES),
    )(field, returned, table.T, skip_weight[0])
    return advanced, mixed.reshape(slots, degrees, 2, channels)


def solution(mesh):
    in_specs = (
        P(("member", "lat"), "lon", None),
        P(),
        P(("lat", "lon"), None, None),
        P(("lat", "lon"), None, None),
        P(),
        P(),
        P(),
    )
    out_specs = (P(("member", "lat"), "lon", None), P(("member", "lat", "lon"), None, None, None))
    body = functools.partial(per_device, mesh.shape["lat"], mesh.shape["lon"])
    return jax.shard_map(body, mesh=mesh, in_specs=in_specs, out_specs=out_specs, check_vma=False)
```
